128 devices in a mesh: vocab: 16 (over x, y), hid: 8 (over z, core).
Axes of the slice: x: 4, y: 4, z: 4, core: 2. Of those that a mesh axis runs over, the one named last changes fastest.
Arguments:
- hidden: bfloat16 [2, 512, 7168], P(None, 'vocab', 'hid'), may hold values from -100 to 100
- head_weight: bfloat16 [7168, 131072], P('hid', 'vocab'), may hold values from -2 to 2
- targets: int32 [2, 512], P(None, 'hid'), may hold values from 0 to 131071
Outputs:
- entropy: float32 [2, 512], P(None, 'hid')
- squared: float32 [2, 512], P(None, 'hid')
The draws below stay inside these ranges and needn't reach their ends.
All inputs are finite; a program needn't handle non-finite values.
Results may differ from the reference program's by a relative error of at most 0.0003.
Values may be sent and summed in bfloat16 or wider, within the bound.
A program may use at most 192 MiB of HBM per device.

```python
import math
import jax
import jax.numpy as jnp

D = 7168
DEPTH = 2
VOCAB = 131072
TOKENS = 512


def column_block(key, index):
    block_key = jax.random.fold_in(jax.random.fold_in(key, 7001), index)
    column_ids = index * 128 + jnp.arange(128)
    column_ramp = 1.0 + 0.25 * column_ids.astype(jnp.float32) / VOCAB
    raw_values = jnp.clip(jax.random.normal(block_key, (D, 128), jnp.float32), -6.0, 6.0)
    return raw_values * column_ramp[None, :] / math.sqrt(D)


def draw_head_weight(key, part):
    blocks = jax.vmap(lambda index: column_block(key, index))(jnp.arange(VOCAB // 128))
    return jnp.transpose(blocks, (1, 0, 2)).reshape(D, VOCAB).astype(jnp.bfloat16)


def draw_hidden(key, part):
    hidden_key = jax.random.fold_in(key, 7002)
    base_values = 3.0 * jnp.clip(jax.random.normal(hidden_key, (DEPTH, TOKENS, D), jnp.float32), -6.0, 6.0)
    return jnp.clip(base_values, -100.0, 100.0).astype(jnp.bfloat16)


def touch_ends(result, rng, smallest, high):
    longest = result.shape.index(max(result.shape))
    spots = []
    for shift in (0, 1):
        where = [jax.random.randint(jax.random.fold_in(rng, axis), (), 0, length) for axis, length in enumerate(result.shape)]
        where[longest] = (where[longest] + shift) % result.shape[longest]
        spots.append(tuple(where))
    return result.at[spots[0]].set(smallest).at[spots[1]].set(high)


def setup_inputs(seed: int = 0) -> dict:
    key_of = jax.random.split(jax.random.key(seed), 4)
    hidden = draw_hidden(jax.random.fold_in(key_of[3], 71), 0)
    head_weight = draw_head_weight(jax.random.fold_in(key_of[3], 71), 0)
    targets = touch_ends(jax.random.randint(key_of[2], (DEPTH, TOKENS), 0, VOCAB), jax.random.fold_in(key_of[2], 1), 0, VOCAB - 1).astype(jnp.int32)
    return dict(hidden=hidden, head_weight=head_weight, targets=targets)


def reference(hidden, head_weight, targets):
    entropy_rows = []
    square_rows = []
    for depth_index in range(DEPTH):
        logits = jnp.dot(hidden[depth_index], head_weight, preferred_element_type=jnp.float32)
        row_peak = jnp.max(logits, axis=1)
        row_total = jnp.sum(jnp.exp(logits - row_peak[:, None]), axis=1)
        log_norm = row_peak + jnp.log(row_total)
        picked = jnp.take_along_axis(logits, targets[depth_index][:, None], axis=1)[:, 0]
        entropy_rows.append(log_norm - picked)
        square_rows.append(log_norm * log_norm)
    return jnp.stack(entropy_rows), jnp.stack(square_rows)
```

```python
import functools
import math

import jax
import jax.numpy as jnp
from jax import lax
from jax.experimental import pallas as pl
from jax.experimental.pallas import tpu as pltpu
from jax.sharding import PartitionSpec as P

MESH = pl.DeviceIdType.MESH
RING = 4
CHUNKS = 4
STEPS = RING * CHUNKS
LAG_FORWARD = 2
LAG_FINAL = 5
LOWEST = -3.0e38


def encode(values, code):
    size = jnp.abs(values)
    square = size * size + 1.0
    level = jnp.log(size + square * lax.rsqrt(square)) * code
    level = jnp.where(values < 0.0, -level, level)
    return jnp.round(level).astype(jnp.int32).astype(jnp.int16)


def decode(codes, code):
    level = codes.astype(jnp.int32).astype(jnp.float32) * (1.0 / code)
    return 0.5 * (jnp.exp(level) - jnp.exp(-level))


def kernel(
    sizes,
    hidden,
    head,
    labels,
    entropy,
    squared,
    weights,
    rows,
    result,
    send_a,
    send_b,
    send_c,
    recv_a,
    recv_b,
    recv_c,
    own,
    pending,
    peaks,
    masses,
    picks,
    label_rows,
    label_tiles,
    stats,
    all_stats,
    local_sem,
    head_local,
    head_send,
    head_recv,
    label_sems,
    row_send,
    row_recv,
    pass_send,
    pass_recv,
    sems_a,
    sems_b,
    sems_c,
    stat_send,
    stat_recv,
):
    block, depth, width, code = sizes
    v, hid = lax.axis_index("vocab"), lax.axis_index("hid")
    x, y = v // RING, v % RING
    z, core = hid // 2, hid % 2
    up, down = (z + 1) % RING, (z + RING - 1) % RING
    partner = (v, z * 2 + 1 - core)
    along = ((v, up * 2 + core), (v, down * 2 + core))
    mine = v * 2 + core
    slot = (x - z + 2 + RING) % RING
    half = 2 * CHUNKS * width

    def row_block(group, place, which):
        return rows.at[
            group,
            pl.ds(pl.multiple_of(place * block, block), block),
            pl.ds(pl.multiple_of(which * depth, 128), depth),
        ]

    def remote(source, target, send, recv, device):
        return pltpu.make_async_remote_copy(
            src_ref=source,
            dst_ref=target,
            send_sem=send,
            recv_sem=recv,
            device_id=device,
            device_id_type=MESH,
        )

    def head_part(which, chunk):
        return weights.at[chunk, pl.ds(pl.multiple_of(which * depth, 16), depth), :]

    def head_columns(which, chunk):
        start = pl.multiple_of(which * half + chunk * width, 128)
        return head.at[:, pl.ds(start, width)]

    order = [d * CHUNKS + i for i in range(CHUNKS) for d in range(2)]

    def load_head(chunk):
        return pltpu.make_async_copy(
            head_columns(core, chunk), head_part(core, chunk), head_local.at[chunk]
        )

    def send_head(chunk):
        return remote(
            head_columns(1 - core, chunk),
            head_part(core, chunk),
            head_send.at[chunk],
            head_recv.at[chunk],
            partner,
        )

    own_rows = pltpu.make_async_copy(hidden, row_block(0, slot, core), local_sem)
    own_rows.start()
    for chunk in order:
        load_head(chunk).start()

    barrier = pltpu.get_barrier_semaphore()

    @pl.loop(1, 32)
    def _(k):
        other = (mine + k) % 32
        pl.semaphore_signal(
            barrier, inc=1, device_id=(other // 2, z * 2 + other % 2), device_id_type=MESH
        )

    for device in along:
        pl.semaphore_signal(barrier, inc=1, device_id=device, device_id_type=MESH)
    pl.semaphore_wait(barrier, 33)

    def send_rows(group, dx):
        device = (((x + dx) % RING) * RING + (y + RING - group) % RING, hid)
        return remote(
            hidden,
            row_block(group, slot, core),
            row_send.at[group, dx],
            row_recv.at[group, slot],
            device,
        )

    own_pass = remote(
        hidden, row_block(0, slot, core), pass_send.at[0, slot], pass_recv.at[0, slot], partner
    )
    own_pass.start()
    for dx in (1, 3, 2):
        send_rows(0, dx).start()
    for chunk in order[:2]:
        send_head(chunk).start()
    for group in range(1, RING):
        for dx in (0, 1, 3, 2):
            send_rows(group, dx).start()

    label_rows[core, 0:1, 0 : block] = labels[0:1, :]
    label_rows[core, 0:1, block : 2 * block] = labels[1:2, :]
    label_copy = remote(
        label_rows.at[core], label_rows.at[core], label_sems.at[0], label_sems.at[1], partner
    )
    label_copy.start()

    def forward_rows(group, place):
        there = row_block(group, place, core)
        return remote(
            there, there, pass_send.at[group, place], pass_recv.at[group, place], partner
        )

    def arrived_rows(group, place):
        there = row_block(group, place, core)
        return remote(there, there, row_send.at[group, 0], row_recv.at[group, place], partner)

    for dx in (1, 3, 2):
        place = (slot + dx) % RING
        arrived_rows(0, place).wait_recv()
        forward_rows(0, place).start()
    for chunk in order[2:]:
        send_head(chunk).start()

    own_rows.wait()
    label_copy.wait()
    for k in range(2):
        label_tiles[k] = jnp.transpose(
            jnp.broadcast_to(label_rows[k, 0:1, :], (2 * block, 2 * block))
        )
        peaks[k] = jnp.full((2 * block, 128), LOWEST, jnp.float32)
        masses[k] = jnp.zeros((2 * block, 128), jnp.float32)
        picks[k] = jnp.zeros((2 * block, 128), jnp.float32)

    def copy_a(t, d):
        return remote(
            send_a.at[t, d], recv_a.at[t, d], sems_a.at[0, t, d], sems_a.at[1, t, d], along[d]
        )

    def copy_b(t, d):
        return remote(
            send_b.at[t, d], recv_b.at[t, d], sems_b.at[0, t, d], sems_b.at[1, t, d], along[1 - d]
        )

    def copy_c(t, d):
        return remote(
            send_c.at[t, d], recv_c.at[t, d], sems_c.at[0, t, d], sems_c.at[1, t, d], along[d]
        )

    def encoded(target, source):
        for r in range(0, block, 16):
            target[r : r + 16, :] = encode(source[r : r + 16, :], code)

    def compute(t):
        group, i = t // CHUNKS, t % CHUNKS

        @pl.when(i == 0)
        def _():
            for place in range(RING):
                there = row_block(group, place, 1 - core)
                remote(
                    there,
                    there,
                    pass_send.at[group, place],
                    pass_recv.at[group, place],
                    partner,
                ).wait_recv()

        @pl.when(group == 0)
        def _():
            for d in range(2):
                chunk = d * CHUNKS + i
                load_head(chunk).wait()
                there = head_part(1 - core, chunk)
                remote(
                    there, there, head_send.at[chunk], head_recv.at[chunk], partner
                ).wait_recv()

        for d in range(2):
            result[d] = jnp.dot(
                rows[group], weights[d * CHUNKS + i], preferred_element_type=jnp.float32
            )
            first, second = (1, 3) if d == 0 else (3, 1)
            encoded(send_a.at[t, d], result.at[d, 0:block, :])
            copy_a(t, d).start()
            encoded(send_b.at[t, d], result.at[d, first * block : (first + 1) * block, :])
            copy_b(t, d).start()
            pending[t, d] = result[d, second * block : (second + 1) * block, :]
            own[t, d] = result[d, 2 * block : 3 * block, :]

        @pl.when((i == CHUNKS - 1) & (group < RING - 1))
        def _():
            for place in range(RING):
                arrived_rows(group + 1, place).wait_recv()
                forward_rows(group + 1, place).start()

    def combine(t):
        for d in range(2):
            copy_a(t, d).wait_recv()
            for r in range(0, block, 16):
                part = slice(r, r + 16)
                send_c[t, d, part, :] = encode(
                    pending[t, d, part, :] + decode(recv_a[t, d, part, :], code), code
                )
            copy_c(t, d).start()

    def finish(t):
        group, i = t // CHUNKS, t % CHUNKS
        source = (y + group) % RING
        which, offset = source // 2, (source % 2) * (block // 2)
        for d in range(2):
            copy_b(t, d).wait_recv()
            copy_c(t, d).wait_recv()
        lane = lax.broadcasted_iota(jnp.int32, (16, 128), 1)
        first = v * (2 * half) + core * half + i * width
        for r in range(0, block, 16):
            token, line = divmod(r, block // 2)
            place = pl.ds(pl.multiple_of(token * block + offset + line, 16), 16)
            gap = label_tiles[which, place, :] - lane - first
            tiles = []
            for d in range(2):
                logits = (
                    own[t, d, r : r + 16, :]
                    + decode(recv_b[t, d, r : r + 16, :], code)
                    + decode(recv_c[t, d, r : r + 16, :], code)
                )
                for j in range(0, width, 128):
                    tiles.append((d * CHUNKS * width + j, logits[:, j : j + 128]))
            before = peaks[which, place, :]
            peak = before
            for _, tile in tiles:
                peak = jnp.maximum(peak, tile)
            mass = masses[which, place, :] * jnp.exp(before - peak)
            pick = picks[which, place, :]
            for shift, tile in tiles:
                mass = mass + jnp.exp(tile - peak)
                pick = pick + jnp.where(gap == shift, tile, 0.0)
            peaks[which, place, :] = peak
            masses[which, place, :] = mass
            picks[which, place, :] = pick
        for d in range(2):
            copy_a(t, d).wait_send()
            copy_b(t, d).wait_send()
            copy_c(t, d).wait_send()

    @pl.loop(0, STEPS + LAG_FINAL)
    def _(t):
        @pl.when(t < STEPS)
        def _():
            compute(t)

        @pl.when((t >= LAG_FORWARD) & (t < STEPS + LAG_FORWARD))
        def _():
            combine(t - LAG_FORWARD)

        @pl.when(t >= LAG_FINAL)
        def _():
            finish(t - LAG_FINAL)

        @pl.when(t == STEPS)
        def _():
            for chunk in range(2 * CHUNKS):
                send_head(chunk).wait_send()
            own_pass.wait_send()
            for dx in (1, 3, 2):
                send_rows(0, dx).wait_send()
                forward_rows(0, (slot + dx) % RING).wait_send()
            for group in range(1, RING):
                for k in range(RING):
                    send_rows(group, k).wait_send()
                    forward_rows(group, k).wait_send()

    for k in range(2):
        peak_lanes = jnp.transpose(peaks[k])
        peak = jnp.max(peak_lanes, axis=0, keepdims=True)
        mass = jnp.sum(
            jnp.transpose(masses[k]) * jnp.exp(peak_lanes - peak), axis=0, keepdims=True
        )
        pick = jnp.sum(jnp.transpose(picks[k]), axis=0, keepdims=True)
        stats[k, 0:1, :] = peak
        stats[k, 1:2, :] = mass
        stats[k, 2:3, :] = pick
        stats[k, 3:8, :] = jnp.zeros((5, 128), jnp.float32)

    def send_stats(k):
        other = (mine + k) % 32
        return remote(
            stats.at[other % 2],
            all_stats.at[mine],
            stat_send.at[k],
            stat_recv.at[mine],
            (other // 2, z * 2 + other % 2),
        )

    @pl.loop(1, 32)
    def _(k):
        send_stats(k).start()

    all_stats[mine] = stats[core]

    @pl.loop(1, 32)
    def _(k):
        other = (mine + k) % 32
        remote(
            stats.at[0], all_stats.at[other], stat_send.at[k], stat_recv.at[other], partner
        ).wait_recv()

    peak = jnp.max(all_stats[:, 0, :], axis=0, keepdims=True)
    mass = jnp.sum(
        all_stats[:, 1, :] * jnp.exp(all_stats[:, 0, :] - peak), axis=0, keepdims=True
    )
    pick = jnp.sum(all_stats[:, 2, :], axis=0, keepdims=True)
    norm = peak + jnp.log(mass)
    loss = norm - pick
    norm = norm * norm
    entropy[0:1, :] = loss[:, 0:block]
    entropy[1:2, :] = loss[:, block : 2 * block]
    squared[0:1, :] = norm[:, 0:block]
    squared[1:2, :] = norm[:, block : 2 * block]

    @pl.loop(1, 32)
    def _(k):
        send_stats(k).wait_send()


def body(hidden, head_weight, targets):
    tokens, depth = hidden.shape[1], hidden.shape[2]
    block = 2 * tokens
    width = head_weight.shape[1] // (4 * CHUNKS)
    bound = 800.0 * depth
    code = 32766.0 / math.asinh(bound)
    piece = (STEPS, 2, block, width)
    coded = pltpu.VMEM(piece, jnp.int16)
    exact = pltpu.VMEM(piece, jnp.float32)
    lanes = pltpu.VMEM((2, 2 * block, 128), jnp.float32)
    dma = pltpu.SemaphoreType.DMA
    out = jax.ShapeDtypeStruct(targets.shape, jnp.float32)
    vmem = pl.BlockSpec(memory_space=pltpu.VMEM)
    hbm = pl.BlockSpec(memory_space=pl.ANY)
    return pl.pallas_call(
        functools.partial(kernel, (block, depth, width, code)),
        out_shape=(out, out),
        in_specs=[hbm, hbm, vmem],
        out_specs=(vmem, vmem),
        scratch_shapes=[
            pltpu.VMEM((2 * CHUNKS, 2 * depth, width), jnp.bfloat16),
            pltpu.VMEM((RING, RING * block, 2 * depth), jnp.bfloat16),
            pltpu.VMEM((2, RING * block, width), jnp.float32),
            coded,
            coded,
            coded,
            coded,
            coded,
            coded,
            exact,
            exact,
            lanes,
            lanes,
            lanes,
            pltpu.VMEM((2, 8, 2 * block), jnp.int32),
            pltpu.VMEM((2, 2 * block, 128), jnp.int32),
            pltpu.VMEM((2, 8, 128), jnp.float32),
            pltpu.VMEM((32, 8, 128), jnp.float32),
            dma,
            dma((2 * CHUNKS,)),
            dma((2 * CHUNKS,)),
            dma((2 * CHUNKS,)),
            dma((2,)),
            dma((RING, RING)),
            dma((RING, RING)),
            dma((RING, RING)),
            dma((RING, RING)),
            dma((2, STEPS, 2)),
            dma((2, STEPS, 2)),
            dma((2, STEPS, 2)),
            dma((32,)),
            dma((32,)),
        ],
        compiler_params=pltpu.CompilerParams(
            collective_id=0, has_side_effects=True, vmem_limit_bytes=62 * 1024 * 1024
        ),
        name="head_loss",
    )(hidden.reshape(block, depth), head_weight, targets)


def solution(mesh):
    return jax.shard_map(
        body,
        mesh=mesh,
        in_specs=(P(None, "vocab", "hid"), P("hid", "vocab"), P(None, "hid")),
        out_specs=(P(None, "hid"), P(None, "hid")),
        check_vma=False,
    )
```

```python
import functools
import math

import jax
import jax.numpy as jnp
from jax import lax
from jax.experimental import pallas as pl
from jax.experimental.pallas import tpu as pltpu
from jax.sharding import PartitionSpec as P

MESH = pl.DeviceIdType.MESH
RING = 4
CHUNKS = 4
STEPS = (RING + 1) * CHUNKS
FIRST = 16
LAG_FORWARD = 3
LAG_FINAL = 7
LOWEST = -3.0e38


def encode(values, code):
    size = jnp.abs(values)
    square = size * size + 1.0
    level = jnp.log(size + square * lax.rsqrt(square)) * code
    level = jnp.where(values < 0.0, -level, level)
    return jnp.round(level).astype(jnp.int32).astype(jnp.int16)


def decode(codes, code):
    level = codes.astype(jnp.int32).astype(jnp.float32) * (1.0 / code)
    return 0.5 * (jnp.exp(level) - jnp.exp(-level))


def kernel(
    sizes,
    hidden,
    head,
    labels,
    log_norm,
    picked,
    weights,
    rows,
    result,
    sent,
    first_part,
    last_parts,
    own,
    pending,
    peaks,
    masses,
    picks,
    label_block,
    label_rows,
    label_tiles,
    stats,
    all_stats,
    label_sems,
    head_local,
    head_recv,
    head_send,
    row_send,
    row_recv,
    column_recv,
    pass_send,
    pass_recv,
    step_send,
    first_recv,
    last_recv,
    stat_sems,
):
    block, depth, width, code = sizes
    v, hid = lax.axis_index("vocab"), lax.axis_index("hid")
    x, y = v // RING, v % RING
    z, core = hid // 2, hid % 2
    partner = (v, z * 2 + 1 - core)
    along = ((v, ((z + 1) % RING) * 2 + core), (v, ((z + RING - 1) % RING) * 2 + core))
    slot = (x - z + 2 + RING) % RING
    half = 2 * CHUNKS * width

    def plane(dx, dy, dc):
        return (((x + dx) % RING) * RING + (y + dy) % RING, z * 2 + (core + dc) % 2)

    def remote(source, target, send, recv, device):
        return pltpu.make_async_remote_copy(
            src_ref=source,
            dst_ref=target,
            send_sem=send,
            recv_sem=recv,
            device_id=device,
            device_id_type=MESH,
        )

    def span(segment):
        return (0, FIRST) if segment == 0 else (FIRST, block - FIRST) if segment == 1 else (0, block)

    def group_of(segment):
        return 0 if isinstance(segment, int) and segment < 2 else segment - 1

    def span_of(segment):
        return span(min(segment, 2) if isinstance(segment, int) else 2)

    def row_block(segment, place, which, blocks=1):
        first, count = span_of(segment)
        start = first * RING + place * count
        return rows.at[
            group_of(segment),
            pl.ds(pl.multiple_of(start, 16), blocks * count),
            pl.ds(pl.multiple_of(which * depth, 128), depth),
        ]

    def source_rows(segment):
        first, count = span_of(segment)
        return hidden.at[pl.ds(first, count), :]

    def head_part(which, i, d, parts=1):
        return weights.at[
            pl.ds(2 * i + d, parts), pl.ds(pl.multiple_of(which * depth, 16), depth), :
        ]

    def head_columns(which, i, d):
        start = pl.multiple_of(which * half + (d * CHUNKS + i) * width, 128)
        return head.at[:, pl.ds(start, width)]

    order = [(i, d) for i in range(CHUNKS) for d in range(2)]

    def load_head(i, d):
        return pltpu.make_async_copy(
            head_columns(core, i, d), head_part(core, i, d).at[0], head_local.at[i]
        )

    def send_head(i, d):
        return remote(
            head_columns(1 - core, i, d),
            head_part(core, i, d).at[0],
            head_send,
            head_recv.at[i],
            partner,
        )

    def here(region, semaphore):
        return pltpu.make_async_copy(region, region, semaphore)

    def arriving(region, semaphore):
        return remote(region, region, head_send, semaphore, partner)

    def leaving(region, semaphore):
        return remote(region, region, semaphore, head_recv.at[0], partner)

    def own_rows(segment):
        return pltpu.make_async_copy(
            source_rows(segment), row_block(segment, slot, core), row_recv.at[segment]
        )

    def column_rows(segment):
        return remote(
            hidden,
            row_block(segment, slot, core),
            row_send.at[segment],
            column_recv.at[segment],
            plane(0, RING + 1 - segment, 0),
        )

    def send_rows(segment, dx):
        there = row_block(segment, slot, core)
        return remote(
            source_rows(segment) if segment < 2 else there,
            there,
            row_send.at[segment],
            row_recv.at[segment],
            plane(dx, 0, 0),
        )

    def relay_rows(segment):
        there = row_block(segment, slot, core)
        arriving(there, column_recv.at[segment]).wait_recv()
        for dx in (2, 1, 3):
            send_rows(segment, dx).start()

    def pass_rows(segment):
        copies = RING if segment < 2 else RING - 1
        arriving(row_block(segment, 0, core, copies), row_recv.at[segment]).wait_recv()
        there = row_block(segment, 0, core, RING)
        remote(there, there, pass_send.at[segment], pass_recv.at[segment], partner).start()

    for segment in range(2):
        own_rows(segment).start()
    load_labels = pltpu.make_async_copy(labels, label_block, label_sems.at[2])
    load_labels.start()
    for part in order:
        load_head(*part).start()

    barrier = pltpu.get_barrier_semaphore()
    others = [
        (dx, dy, dc) for dy in range(RING) for dx in range(RING) for dc in range(2) if dx or dy or dc
    ]
    with jax.named_scope("barrier"):
        near = [plane(2, 0, 0), plane(1, 0, 0), plane(3, 0, 0), plane(0, 0, 1), *along]
        far = [plane(*o) for o in others if o[1] or (o[0] and o[2])]
        for device in near + far:
            pl.semaphore_signal(barrier, inc=1, device_id=device, device_id_type=MESH)
        pl.semaphore_wait(barrier, len(near + far))

    for dx in (2, 1, 3):
        send_rows(0, dx).start()
    for part in order[:3]:
        send_head(*part).start()
    for dx in (2, 1, 3):
        send_rows(1, dx).start()
    for segment in (2, 4, 3):
        column_rows(segment).start()

    load_labels.wait()
    label_rows[core, 0:1, 0:block] = label_block[0:1, :]
    label_rows[core, 0:1, block : 2 * block] = label_block[1:2, :]
    label_copy = remote(
        label_rows.at[core], label_rows.at[core], label_sems.at[0], label_sems.at[1], partner
    )
    label_copy.start()
    for k in range(2):
        peaks[k] = jnp.full((2 * block, 128), LOWEST, jnp.float32)
        masses[k] = jnp.zeros((2 * block, 128), jnp.float32)
        picks[k] = jnp.zeros((2 * block, 128), jnp.float32)

    with jax.named_scope("rows"):
        pass_rows(0)
    relay_rows(2)
    for part in order[3:6]:
        send_head(*part).start()

    def send_part(t, d, count, which):
        part = pl.ds(0, count)
        if which == 0:
            target, semaphore = first_part.at[t, d, part], first_recv.at[t]
        else:
            target, semaphore = last_parts.at[t, which - 1, d, part], last_recv.at[t]
        device = along[1 - d] if which == 1 else along[d]
        return remote(sent.at[t, which, d, part], target, step_send.at[t], semaphore, device)

    def compute(t, i, segment):
        first, count = span_of(segment)
        early = isinstance(segment, int)

        @pl.when(i == 0)
        @jax.named_scope("wait_rows")
        def _():
            region = row_block(segment, 0, 1 - core, RING)
            arriving(region, pass_recv.at[segment]).wait_recv()

        if early and segment == 0:
            with jax.named_scope("wait_head"):
                here(head_part(core, i, 0, 2), head_local.at[i]).wait()
                arriving(head_part(1 - core, i, 0, 2), head_recv.at[i]).wait_recv()

        for d in range(2):
            result[d, 0 : RING * count, :] = jnp.dot(
                rows[group_of(segment), first * RING : (first + count) * RING, :],
                weights[2 * i + d],
                preferred_element_type=jnp.float32,
            )
            near, far = (1, 3) if d == 0 else (3, 1)
            for which, at in ((0, 0), (1, near * count)):
                for r in range(0, count, 16):
                    sent[t, which, d, r : r + 16, :] = encode(
                        result[d, at + r : at + r + 16, :], code
                    )
                send_part(t, d, count, which).start()
            pending[t, d, 0:count, :] = result[d, far * count : (far + 1) * count, :]
            own[t, d, 0:count, :] = result[d, 2 * count : 3 * count, :]

    def combine(t, i, segment):
        _, count = span_of(segment)
        with jax.named_scope("wait_a"):
            arriving(first_part.at[t, :, pl.ds(0, count)], first_recv.at[t]).wait_recv()
        for d in range(2):
            for r in range(0, count, 16):
                part = slice(r, r + 16)
                sent[t, 2, d, part, :] = encode(
                    pending[t, d, part, :] + decode(first_part[t, d, part, :], code), code
                )
            send_part(t, d, count, 2).start()

    def finish(t, i, segment):
        first, count = span_of(segment)
        source = (y + group_of(segment)) % RING
        which, offset = source // 2, (source % 2) * (block // 2)
        with jax.named_scope("wait_bc"):
            arriving(last_parts.at[t, :, :, pl.ds(0, count)], last_recv.at[t]).wait_recv()
        lane = lax.broadcasted_iota(jnp.int32, (16, 128), 1)
        column = v * (2 * half) + core * half + i * width
        for r in range(0, count, 16):
            token, line = divmod(first + r, block // 2)
            place = pl.ds(pl.multiple_of(token * block + offset + line, 16), 16)
            gap = label_tiles[which, place, :] - lane - column
            tiles = []
            for d in range(2):
                logits = (
                    own[t, d, r : r + 16, :]
                    + decode(last_parts[t, 0, d, r : r + 16, :], code)
                    + decode(last_parts[t, 1, d, r : r + 16, :], code)
                )
                for j in range(0, width, 128):
                    tiles.append((d * CHUNKS * width + j, logits[:, j : j + 128]))
            before = peaks[which, place, :]
            peak = before
            for _, tile in tiles:
                peak = jnp.maximum(peak, tile)
            mass = masses[which, place, :] * jnp.exp(before - peak)
            pick = picks[which, place, :]
            for shift, tile in tiles:
                mass = mass + jnp.exp(tile - peak)
                pick = pick + jnp.where(gap == shift, tile, 0.0)
            peaks[which, place, :] = peak
            masses[which, place, :] = mass
            picks[which, place, :] = pick
        leaving(sent.at[t, :, :, pl.ds(0, count)], step_send.at[t]).wait_send()

    def each(stage, name, t):
        early = (t >= 0) & (t < 2 * CHUNKS)
        is_first = (t < 3) | (t == 5)

        @pl.when(early & is_first)
        @jax.named_scope(name + "0")
        def _():
            stage(t, jnp.minimum(t, 3), 0)

        @pl.when(early & jnp.logical_not(is_first))
        @jax.named_scope(name + "1")
        def _():
            stage(t, jnp.where(t < 5, t - 3, t - 4), 1)

        @pl.when((t >= 2 * CHUNKS) & (t < STEPS))
        @jax.named_scope(name)
        def _():
            stage(t, t % CHUNKS, t // CHUNKS)

    @pl.loop(0, STEPS + LAG_FINAL)
    def _(t):
        each(compute, "compute", t)
        each(combine, "combine", t - LAG_FORWARD)

        @pl.when(t == 4)
        @jax.named_scope("labels")
        def _():
            label_copy.wait()
            for k in range(2):
                label_tiles[k] = jnp.transpose(
                    jnp.broadcast_to(label_rows[k, 0:1, :], (2 * block, 2 * block))
                )

        each(finish, "finish", t - LAG_FINAL)

        @pl.when(t == 1)
        @jax.named_scope("pass1")
        def _():
            pass_rows(1)
            for part in order[6:]:
                send_head(*part).start()

        for step, stage, segment in (
            (5, relay_rows, 3),
            (6, pass_rows, 2),
            (9, relay_rows, 4),
            (10, pass_rows, 3),
            (14, pass_rows, 4),
        ):

            @pl.when(t == step)
            @jax.named_scope(stage.__name__)
            def _():
                stage(segment)

        @pl.when(t == STEPS)
        @jax.named_scope("drain")
        def _():
            leaving(weights.at[:, pl.ds(0, depth), :], head_send).wait_send()
            for segment in range(RING + 1):
                copies = RING - 1 if segment < 2 else RING
                leaving(row_block(segment, 0, core, copies), row_send.at[segment]).wait_send()
                leaving(row_block(segment, 0, core, RING), pass_send.at[segment]).wait_send()

    with jax.named_scope("reduce"):
        for k in range(2):
            peak_lanes = jnp.transpose(peaks[k])
            peak = jnp.max(peak_lanes, axis=0, keepdims=True)
            mass = jnp.sum(
                jnp.transpose(masses[k]) * jnp.exp(peak_lanes - peak), axis=0, keepdims=True
            )
            pick = jnp.sum(jnp.transpose(picks[k]), axis=0, keepdims=True)
            stats[k, 0:1, :] = peak
            stats[k, 1:2, :] = mass
            stats[k, 2:3, :] = pick
            stats[k, 3:4, :] = jnp.zeros((1, 128), jnp.float32)

    def number(dx, dy, dc):
        return (dx * RING + dy) * 2 + dc

    def send_stats(dx, dy, dc):
        back = number((RING - dx) % RING, (RING - dy) % RING, dc)
        return remote(
            stats.at[(core + dc) % 2],
            all_stats.at[back],
            stat_sems.at[0],
            stat_sems.at[1],
            plane(dx, dy, dc),
        )

    def hops(offset):
        return sum(min(o, RING - o) for o in offset[:2])

    with jax.named_scope("send_stats"):
        for offset in sorted(others, key=hops, reverse=True):
            send_stats(*offset).start()
        all_stats[0] = stats[core]
        leaving(all_stats.at[pl.ds(1, 31)], stat_sems.at[0]).wait_send()

    with jax.named_scope("wait_stats"):
        arriving(all_stats.at[pl.ds(1, 31)], stat_sems.at[1]).wait_recv()

    with jax.named_scope("merge"):
        peak = jnp.max(all_stats[:, 0, :], axis=0, keepdims=True)
        mass = jnp.sum(
            all_stats[:, 1, :] * jnp.exp(all_stats[:, 0, :] - peak), axis=0, keepdims=True
        )
        pick = jnp.sum(all_stats[:, 2, :], axis=0, keepdims=True)
        norm = peak + jnp.log(mass)
        for k in range(2):
            log_norm[k : k + 1, :] = norm[:, k * block : (k + 1) * block]
            picked[k : k + 1, :] = pick[:, k * block : (k + 1) * block]


def body(hidden, head_weight, targets):
    tokens, depth = hidden.shape[1], hidden.shape[2]
    block = 2 * tokens
    width = head_weight.shape[1] // (4 * CHUNKS)
    bound = 800.0 * depth
    code = 32766.0 / math.asinh(bound)
    piece = (2, block, width)
    exact = pltpu.VMEM((STEPS, *piece), jnp.float32)
    lanes = pltpu.VMEM((2, 2 * block, 128), jnp.float32)
    dma = pltpu.SemaphoreType.DMA
    out = jax.ShapeDtypeStruct(targets.shape, jnp.float32)
    vmem = pl.BlockSpec(memory_space=pltpu.VMEM)
    hbm = pl.BlockSpec(memory_space=pltpu.HBM)
    in_hbm = functools.partial(pltpu.with_memory_space_constraint, memory_space=pltpu.HBM)
    log_norm, picked = pl.pallas_call(
        functools.partial(kernel, (block, depth, width, code)),
        out_shape=(out, out),
        in_specs=[hbm, hbm, hbm],
        out_specs=(vmem, vmem),
        scratch_shapes=[
            pltpu.VMEM((2 * CHUNKS, 2 * depth, width), jnp.bfloat16),
            pltpu.VMEM((RING, RING * block, 2 * depth), jnp.bfloat16),
            pltpu.VMEM((2, RING * block, width), jnp.float32),
            pltpu.VMEM((STEPS, 3, *piece), jnp.int16),
            pltpu.VMEM((STEPS, *piece), jnp.int16),
            pltpu.VMEM((STEPS, 2, *piece), jnp.int16),
            exact,
            exact,
            lanes,
            lanes,
            lanes,
            pltpu.VMEM(targets.shape, jnp.int32),
            pltpu.VMEM((2, 8, 2 * block), jnp.int32),
            pltpu.VMEM((2, 2 * block, 128), jnp.int32),
            pltpu.VMEM((2, 4, 128), jnp.float32),
            pltpu.VMEM((32, 4, 128), jnp.float32),
            dma((3,)),
            dma((CHUNKS,)),
            dma((CHUNKS,)),
            dma,
            dma((RING + 1,)),
            dma((RING + 1,)),
            dma((RING + 1,)),
            dma((RING + 1,)),
            dma((RING + 1,)),
            dma((STEPS,)),
            dma((STEPS,)),
            dma((STEPS,)),
            dma((2,)),
        ],
        compiler_params=pltpu.CompilerParams(
            collective_id=0, has_side_effects=True, vmem_limit_bytes=50 * 1024 * 1024
        ),
        name="head_loss",
    )(in_hbm(hidden.reshape(block, depth)), head_weight, in_hbm(targets))
    return log_norm - picked, log_norm * log_norm


def solution(mesh):
    return jax.shard_map(
        body,
        mesh=mesh,
        in_specs=(P(None, "vocab", "hid"), P("hid", "vocab"), P(None, "hid")),
        out_specs=(P(None, "hid"), P(None, "hid")),
        check_vma=False,
    )
```

```python
import functools
import math

import jax
import jax.numpy as jnp
from jax import lax
from jax.experimental import pallas as pl
from jax.experimental.pallas import tpu as pltpu
from jax.sharding import PartitionSpec as P

MESH = pl.DeviceIdType.MESH
RING = 4
CHUNKS = 4
STEPS = (RING + 1) * CHUNKS
FIRST = 32
LAG_FORWARD = 3
LAG_FINAL = 7
LOWEST = -3.0e38


def encode(values, code):
    size = jnp.abs(values)
    square = size * size + 1.0
    level = jnp.log(size + square * lax.rsqrt(square)) * code
    level = jnp.where(values < 0.0, -level, level)
    return jnp.round(level).astype(jnp.int32).astype(jnp.int16)


def decode(codes, code):
    level = codes.astype(jnp.int32).astype(jnp.float32) * (1.0 / code)
    return 0.5 * (jnp.exp(level) - jnp.exp(-level))


def kernel(
    sizes,
    hidden,
    head,
    labels,
    log_norm,
    picked,
    weights,
    rows,
    result,
    sent,
    first_part,
    last_parts,
    own,
    pending,
    peaks,
    masses,
    picks,
    label_block,
    label_rows,
    label_tiles,
    stats,
    all_stats,
    label_sems,
    head_local,
    head_recv,
    head_send,
    own_sem,
    row_send,
    row_recv,
    column_recv,
    pass_send,
    pass_recv,
    step_send,
    first_recv,
    last_recv,
    stat_sems,
):
    block, depth, width, code = sizes
    v, hid = lax.axis_index("vocab"), lax.axis_index("hid")
    x, y = v // RING, v % RING
    z, core = hid // 2, hid % 2
    partner = (v, z * 2 + 1 - core)
    along = ((v, ((z + 1) % RING) * 2 + core), (v, ((z + RING - 1) % RING) * 2 + core))
    slot = (x - z + 2 + RING) % RING
    half = 2 * CHUNKS * width

    def plane(dx, dy, dc):
        return (((x + dx) % RING) * RING + (y + dy) % RING, z * 2 + (core + dc) % 2)

    def remote(source, target, send, recv, device):
        return pltpu.make_async_remote_copy(
            src_ref=source,
            dst_ref=target,
            send_sem=send,
            recv_sem=recv,
            device_id=device,
            device_id_type=MESH,
        )

    def span(segment):
        return (0, FIRST) if segment == 0 else (FIRST, block - FIRST) if segment == 1 else (0, block)

    def group_of(segment):
        return 0 if isinstance(segment, int) and segment < 2 else segment - 1

    def span_of(segment):
        return span(min(segment, 2) if isinstance(segment, int) else 2)

    def row_block(segment, place, which, blocks=1):
        first, count = span_of(segment)
        start = first * RING + place * count
        return rows.at[
            group_of(segment),
            pl.ds(pl.multiple_of(start, 16), blocks * count),
            pl.ds(pl.multiple_of(which * depth, 128), depth),
        ]

    def source_rows(segment):
        first, count = span_of(segment)
        return hidden.at[pl.ds(first, count), :]

    def head_part(which, i, d, parts=1):
        return weights.at[
            pl.ds(2 * i + d, parts), pl.ds(pl.multiple_of(which * depth, 16), depth), :
        ]

    def head_columns(which, i, d):
        start = pl.multiple_of(which * half + (d * CHUNKS + i) * width, 128)
        return head.at[:, pl.ds(start, width)]

    order = [(i, d) for i in range(CHUNKS) for d in range(2)]

    def load_head(i, d):
        return pltpu.make_async_copy(
            head_columns(core, i, d), head_part(core, i, d).at[0], head_local.at[i]
        )

    def send_head(i, d):
        return remote(
            head_columns(1 - core, i, d),
            head_part(core, i, d).at[0],
            head_send,
            head_recv.at[i],
            partner,
        )

    def here(region, semaphore):
        return pltpu.make_async_copy(region, region, semaphore)

    def arriving(region, semaphore):
        return remote(region, region, head_send, semaphore, partner)

    def leaving(region, semaphore):
        return remote(region, region, semaphore, head_recv.at[0], partner)

    def own_rows(segment):
        return pltpu.make_async_copy(
            source_rows(segment), row_block(segment, slot, core), own_sem.at[segment]
        )

    def column_rows(segment, part):
        first, count = span(part)
        return remote(
            row_block(part, slot, core),
            rows.at[
                group_of(segment),
                pl.ds(pl.multiple_of(slot * block + first, 16), count),
                pl.ds(pl.multiple_of(core * depth, 128), depth),
            ],
            row_send.at[segment],
            column_recv.at[segment],
            plane(0, RING + 1 - segment, 0),
        )

    def send_rows(segment, dx):
        there = row_block(segment, slot, core)
        return remote(
            there,
            there,
            row_send.at[segment],
            row_recv.at[segment],
            plane(dx, 0, 0),
        )

    def relay_rows(segment):
        there = row_block(segment, slot, core)
        arriving(there, column_recv.at[segment]).wait_recv()
        for dx in (2, 1, 3):
            send_rows(segment, dx).start()

    def pass_rows(segment):
        arriving(row_block(segment, 0, core, RING - 1), row_recv.at[segment]).wait_recv()
        there = row_block(segment, 0, core, RING)
        remote(there, there, pass_send.at[segment], pass_recv.at[segment], partner).start()

    for segment in range(2):
        own_rows(segment).start()
    load_labels = pltpu.make_async_copy(labels, label_block, label_sems.at[2])
    load_labels.start()
    for part in order:
        load_head(*part).start()

    barrier = pltpu.get_barrier_semaphore()
    others = [
        (dx, dy, dc) for dy in range(RING) for dx in range(RING) for dc in range(2) if dx or dy or dc
    ]
    with jax.named_scope("barrier"):
        near = [plane(2, 0, 0), plane(1, 0, 0), plane(3, 0, 0), plane(0, 0, 1), *along]
        near += [plane(0, 2, 0), plane(0, 1, 0), plane(0, 3, 0)]
        for device in near:
            pl.semaphore_signal(barrier, inc=1, device_id=device, device_id_type=MESH)
        pl.semaphore_wait(barrier, len(near))

    own_rows(0).wait()
    own_rows(1).wait()
    for dx in (2, 1, 3):
        send_rows(0, dx).start()
    for part in order[:3]:
        send_head(*part).start()
    for dx in (2, 1, 3):
        send_rows(1, dx).start()
    for segment in (2, 4, 3):
        for part in range(2):
            column_rows(segment, part).start()

    load_labels.wait()
    label_rows[core, 0:1, 0:block] = label_block[0:1, :]
    label_rows[core, 0:1, block : 2 * block] = label_block[1:2, :]
    label_copy = remote(
        label_rows.at[core], label_rows.at[core], label_sems.at[0], label_sems.at[1], partner
    )
    label_copy.start()
    for k in range(2):
        peaks[k] = jnp.full((2 * block, 128), LOWEST, jnp.float32)
        masses[k] = jnp.zeros((2 * block, 128), jnp.float32)
        picks[k] = jnp.zeros((2 * block, 128), jnp.float32)

    with jax.named_scope("rows"):
        pass_rows(0)
    relay_rows(2)
    for part in order[3:4]:
        send_head(*part).start()

    def send_part(t, d, count, which):
        part = pl.ds(0, count)
        if which == 0:
            target, semaphore = first_part.at[t, d, part], first_recv.at[t]
        else:
            target, semaphore = last_parts.at[t, which - 1, d, part], last_recv.at[t]
        device = along[1 - d] if which == 1 else along[d]
        return remote(sent.at[t, which, d, part], target, step_send.at[t], semaphore, device)

    def compute(t, i, segment):
        first, count = span_of(segment)
        early = isinstance(segment, int)

        @pl.when(i == 0)
        @jax.named_scope("wait_rows")
        def _():
            region = row_block(segment, 0, 1 - core, RING)
            arriving(region, pass_recv.at[segment]).wait_recv()

        if early and segment == 0:
            with jax.named_scope("wait_head"):
                here(head_part(core, i, 0, 2), head_local.at[i]).wait()
                arriving(head_part(1 - core, i, 0, 2), head_recv.at[i]).wait_recv()

        for d in range(2):
            result[d, 0 : RING * count, :] = jnp.dot(
                rows[group_of(segment), first * RING : (first + count) * RING, :],
                weights[2 * i + d],
                preferred_element_type=jnp.float32,
            )
            near, far = (1, 3) if d == 0 else (3, 1)
            for which, at in ((0, 0), (1, near * count)):
                for r in range(0, count, 16):
                    sent[t, which, d, r : r + 16, :] = encode(
                        result[d, at + r : at + r + 16, :], code
                    )
                send_part(t, d, count, which).start()
            pending[t, d, 0:count, :] = result[d, far * count : (far + 1) * count, :]
            own[t, d, 0:count, :] = result[d, 2 * count : 3 * count, :]

    def combine(t, i, segment):
        _, count = span_of(segment)
        with jax.named_scope("wait_a"):
            arriving(first_part.at[t, :, pl.ds(0, count)], first_recv.at[t]).wait_recv()
        for d in range(2):
            for r in range(0, count, 16):
                part = slice(r, r + 16)
                sent[t, 2, d, part, :] = encode(
                    pending[t, d, part, :] + decode(first_part[t, d, part, :], code), code
                )
            send_part(t, d, count, 2).start()

    def finish(t, i, segment):
        first, count = span_of(segment)
        source = (y + group_of(segment)) % RING
        which, offset = source // 2, (source % 2) * (block // 2)
        with jax.named_scope("wait_bc"):
            arriving(last_parts.at[t, :, :, pl.ds(0, count)], last_recv.at[t]).wait_recv()
        lane = lax.broadcasted_iota(jnp.int32, (16, 128), 1)
        column = v * (2 * half) + core * half + i * width
        for r in range(0, count, 16):
            token, line = divmod(first + r, block // 2)
            place = pl.ds(pl.multiple_of(token * block + offset + line, 16), 16)
            gap = label_tiles[which, place, :] - lane - column
            tiles = []
            for d in range(2):
                logits = (
                    own[t, d, r : r + 16, :]
                    + decode(last_parts[t, 0, d, r : r + 16, :], code)
                    + decode(last_parts[t, 1, d, r : r + 16, :], code)
                )
                for j in range(0, width, 128):
                    tiles.append((d * CHUNKS * width + j, logits[:, j : j + 128]))
            before = peaks[which, place, :]
            peak = before
            for _, tile in tiles:
                peak = jnp.maximum(peak, tile)
            mass = masses[which, place, :] * jnp.exp(before - peak)
            pick = picks[which, place, :]
            for shift, tile in tiles:
                mass = mass + jnp.exp(tile - peak)
                pick = pick + jnp.where(gap == shift, tile, 0.0)
            peaks[which, place, :] = peak
            masses[which, place, :] = mass
            picks[which, place, :] = pick
        leaving(sent.at[t, :, :, pl.ds(0, count)], step_send.at[t]).wait_send()

    def each(stage, name, t):
        early = (t >= 0) & (t < 2 * CHUNKS)
        is_first = (t < 2) | (t == 4) | (t == 6)

        @pl.when(early & is_first)
        @jax.named_scope(name + "0")
        def _():
            stage(t, jnp.where(t < 2, t, t // 2), 0)

        @pl.when(early & jnp.logical_not(is_first))
        @jax.named_scope(name + "1")
        def _():
            stage(t, jnp.where(t < 4, t - 2, t // 2), 1)

        @pl.when((t >= 2 * CHUNKS) & (t < STEPS))
        @jax.named_scope(name)
        def _():
            stage(t, t % CHUNKS, t // CHUNKS)

    @pl.loop(0, STEPS + LAG_FINAL)
    def _(t):
        each(compute, "compute", t)
        each(combine, "combine", t - LAG_FORWARD)

        @pl.when(t == 4)
        @jax.named_scope("labels")
        def _():
            label_copy.wait()
            for k in range(2):
                label_tiles[k] = jnp.transpose(
                    jnp.broadcast_to(label_rows[k, 0:1, :], (2 * block, 2 * block))
                )

        each(finish, "finish", t - LAG_FINAL)

        @pl.when(t == 0)
        @jax.named_scope("pass1")
        def _():
            pass_rows(1)
            for part in order[4:]:
                send_head(*part).start()

        for step, stage, segment in (
            (5, relay_rows, 3),
            (6, pass_rows, 2),
            (9, relay_rows, 4),
            (10, pass_rows, 3),
            (14, pass_rows, 4),
        ):

            @pl.when(t == step)
            @jax.named_scope(stage.__name__)
            def _():
                stage(segment)

        @pl.when(t == STEPS)
        @jax.named_scope("drain")
        def _():
            leaving(weights.at[:, pl.ds(0, depth), :], head_send).wait_send()
            for segment in range(RING + 1):
                copies = RING - 1 if segment < 2 else RING
                leaving(row_block(segment, 0, core, copies), row_send.at[segment]).wait_send()
                leaving(row_block(segment, 0, core, RING), pass_send.at[segment]).wait_send()

    with jax.named_scope("reduce"):
        for k in range(2):
            peak_lanes = jnp.transpose(peaks[k])
            peak = jnp.max(peak_lanes, axis=0, keepdims=True)
            mass = jnp.sum(
                jnp.transpose(masses[k]) * jnp.exp(peak_lanes - peak), axis=0, keepdims=True
            )
            pick = jnp.sum(jnp.transpose(picks[k]), axis=0, keepdims=True)
            stats[k, 0:1, :] = peak
            stats[k, 1:2, :] = mass
            stats[k, 2:3, :] = pick
            stats[k, 3:4, :] = jnp.zeros((1, 128), jnp.float32)

    def number(dx, dy, dc):
        return (dx * RING + dy) * 2 + dc

    def send_stats(dx, dy, dc):
        back = number((RING - dx) % RING, (RING - dy) % RING, dc)
        return remote(
            stats.at[(core + dc) % 2],
            all_stats.at[back],
            stat_sems.at[0],
            stat_sems.at[1],
            plane(dx, dy, dc),
        )

    def hops(offset):
        return sum(min(o, RING - o) for o in offset[:2])

    with jax.named_scope("send_stats"):
        for offset in sorted(others, key=hops, reverse=True):
            send_stats(*offset).start()
        all_stats[0] = stats[core]
        leaving(all_stats.at[pl.ds(1, 31)], stat_sems.at[0]).wait_send()

    with jax.named_scope("wait_stats"):
        arriving(all_stats.at[pl.ds(1, 31)], stat_sems.at[1]).wait_recv()

    with jax.named_scope("merge"):
        peak = jnp.max(all_stats[:, 0, :], axis=0, keepdims=True)
        mass = jnp.sum(
            all_stats[:, 1, :] * jnp.exp(all_stats[:, 0, :] - peak), axis=0, keepdims=True
        )
        pick = jnp.sum(all_stats[:, 2, :], axis=0, keepdims=True)
        norm = peak + jnp.log(mass)
        for k in range(2):
            log_norm[k : k + 1, :] = norm[:, k * block : (k + 1) * block]
            picked[k : k + 1, :] = pick[:, k * block : (k + 1) * block]


def body(hidden, head_weight, targets):
    tokens, depth = hidden.shape[1], hidden.shape[2]
    block = 2 * tokens
    width = head_weight.shape[1] // (4 * CHUNKS)
    bound = 800.0 * depth
    code = 32766.0 / math.asinh(bound)
    piece = (2, block, width)
    exact = pltpu.VMEM((STEPS, *piece), jnp.float32)
    lanes = pltpu.VMEM((2, 2 * block, 128), jnp.float32)
    dma = pltpu.SemaphoreType.DMA
    out = jax.ShapeDtypeStruct(targets.shape, jnp.float32)
    vmem = pl.BlockSpec(memory_space=pltpu.VMEM)
    hbm = pl.BlockSpec(memory_space=pltpu.HBM)
    in_hbm = functools.partial(pltpu.with_memory_space_constraint, memory_space=pltpu.HBM)
    log_norm, picked = pl.pallas_call(
        functools.partial(kernel, (block, depth, width, code)),
        out_shape=(out, out),
        in_specs=[hbm, hbm, hbm],
        out_specs=(vmem, vmem),
        scratch_shapes=[
            pltpu.VMEM((2 * CHUNKS, 2 * depth, width), jnp.bfloat16),
            pltpu.VMEM((RING, RING * block, 2 * depth), jnp.bfloat16),
            pltpu.VMEM((2, RING * block, width), jnp.float32),
            pltpu.VMEM((STEPS, 3, *piece), jnp.int16),
            pltpu.VMEM((STEPS, *piece), jnp.int16),
            pltpu.VMEM((STEPS, 2, *piece), jnp.int16),
            exact,
            exact,
            lanes,
            lanes,
            lanes,
            pltpu.VMEM(targets.shape, jnp.int32),
            pltpu.VMEM((2, 8, 2 * block), jnp.int32),
            pltpu.VMEM((2, 2 * block, 128), jnp.int32),
            pltpu.VMEM((2, 4, 128), jnp.float32),
            pltpu.VMEM((32, 4, 128), jnp.float32),
            dma((3,)),
            dma((CHUNKS,)),
            dma((CHUNKS,)),
            dma,
            dma((2,)),
            dma((RING + 1,)),
            dma((RING + 1,)),
            dma((RING + 1,)),
            dma((RING + 1,)),
            dma((RING + 1,)),
            dma((STEPS,)),
            dma((STEPS,)),
            dma((STEPS,)),
            dma((2,)),
        ],
        compiler_params=pltpu.CompilerParams(
            collective_id=0, has_side_effects=True, vmem_limit_bytes=50 * 1024 * 1024
        ),
        name="head_loss",
    )(in_hbm(hidden.reshape(block, depth)), head_weight, in_hbm(targets))
    return log_norm - picked, log_norm * log_norm


def solution(mesh):
    return jax.shard_map(
        body,
        mesh=mesh,
        in_specs=(P(None, "vocab", "hid"), P("hid", "vocab"), P(None, "hid")),
        out_specs=(P(None, "hid"), P(None, "hid")),
        check_vma=False,
    )
```

```python
import functools
import math

import jax
import jax.numpy as jnp
from jax import lax
from jax.experimental import pallas as pl
from jax.experimental.pallas import tpu as pltpu
from jax.sharding import PartitionSpec as P

MESH = pl.DeviceIdType.MESH
RING = 4
CHUNKS = 4
STEPS = (RING + 1) * CHUNKS
FIRST = 32
EARLY = 3
LATE = 1
LAG_FORWARD = 3
LAG_FINAL = 7
LOWEST = -3.0e38


def encode(values, code):
    size = jnp.abs(values)
    square = size * size + 1.0
    level = jnp.log(size + square * lax.rsqrt(square)) * code
    level = jnp.where(values < 0.0, -level, level)
    return jnp.round(level).astype(jnp.int32).astype(jnp.int16)


def decode(codes, code):
    level = codes.astype(jnp.int32).astype(jnp.float32) * (1.0 / code)
    return 0.5 * (jnp.exp(level) - jnp.exp(-level))


def kernel(
    sizes,
    hidden,
    head,
    labels,
    log_norm,
    picked,
    weights,
    rows,
    result,
    sent,
    first_part,
    last_parts,
    own,
    pending,
    peaks,
    masses,
    picks,
    label_block,
    label_rows,
    label_tiles,
    stats,
    all_stats,
    label_sems,
    head_local,
    head_recv,
    head_send,
    own_sem,
    row_send,
    row_recv,
    column_recv,
    pass_send,
    pass_recv,
    step_send,
    first_recv,
    last_recv,
    stat_sems,
):
    block, depth, width, code = sizes
    v, hid = lax.axis_index("vocab"), lax.axis_index("hid")
    x, y = v // RING, v % RING
    z, core = hid // 2, hid % 2
    partner = (v, z * 2 + 1 - core)
    along = ((v, ((z + 1) % RING) * 2 + core), (v, ((z + RING - 1) % RING) * 2 + core))
    slot = (x - z + 2 + RING) % RING
    half = 2 * CHUNKS * width

    def plane(dx, dy, dc):
        return (((x + dx) % RING) * RING + (y + dy) % RING, z * 2 + (core + dc) % 2)

    def remote(source, target, send, recv, device):
        return pltpu.make_async_remote_copy(
            src_ref=source,
            dst_ref=target,
            send_sem=send,
            recv_sem=recv,
            device_id=device,
            device_id_type=MESH,
        )

    def span(segment):
        return (0, FIRST) if segment == 0 else (FIRST, block - FIRST) if segment == 1 else (0, block)

    def group_of(segment):
        return 0 if isinstance(segment, int) and segment < 2 else segment - 1

    def span_of(segment):
        return span(min(segment, 2) if isinstance(segment, int) else 2)

    def row_block(segment, place, which, blocks=1):
        first, count = span_of(segment)
        start = first * RING + place * count
        return rows.at[
            group_of(segment),
            pl.ds(pl.multiple_of(start, 16), blocks * count),
            pl.ds(pl.multiple_of(which * depth, 128), depth),
        ]

    def source_rows(segment):
        first, count = span_of(segment)
        return hidden.at[pl.ds(first, count), :]

    def head_part(which, i, d, parts=1):
        return weights.at[
            pl.ds(2 * i + d, parts), pl.ds(pl.multiple_of(which * depth, 16), depth), :
        ]

    def head_columns(which, i, d):
        start = pl.multiple_of(which * half + (d * CHUNKS + i) * width, 128)
        return head.at[:, pl.ds(start, width)]

    order = [(i, d) for i in range(CHUNKS) for d in range(2)]

    def load_head(i, d):
        return pltpu.make_async_copy(
            head_columns(core, i, d), head_part(core, i, d).at[0], head_local.at[i]
        )

    def send_head(i, d):
        return remote(
            head_columns(1 - core, i, d),
            head_part(core, i, d).at[0],
            head_send,
            head_recv.at[i],
            partner,
        )

    def here(region, semaphore):
        return pltpu.make_async_copy(region, region, semaphore)

    def arriving(region, semaphore):
        return remote(region, region, head_send, semaphore, partner)

    def leaving(region, semaphore):
        return remote(region, region, semaphore, head_recv.at[0], partner)

    def own_rows(segment):
        return pltpu.make_async_copy(
            source_rows(segment), row_block(segment, slot, core), own_sem.at[segment]
        )

    def column_rows(segment, part):
        first, count = span(part)
        return remote(
            row_block(part, slot, core),
            rows.at[
                group_of(segment),
                pl.ds(pl.multiple_of(slot * block + first, 16), count),
                pl.ds(pl.multiple_of(core * depth, 128), depth),
            ],
            row_send.at[segment],
            column_recv.at[segment],
            plane(0, RING + 1 - segment, 0),
        )

    def send_rows(segment, dx):
        there = row_block(segment, slot, core)
        return remote(
            there,
            there,
            row_send.at[segment],
            row_recv.at[segment],
            plane(dx, 0, 0),
        )

    def relay_rows(segment):
        there = row_block(segment, slot, core)
        arriving(there, column_recv.at[segment]).wait_recv()
        for dx in (2, 1, 3):
            send_rows(segment, dx).start()

    def pass_rows(segment):
        arriving(row_block(segment, 0, core, RING - 1), row_recv.at[segment]).wait_recv()
        there = row_block(segment, 0, core, RING)
        remote(there, there, pass_send.at[segment], pass_recv.at[segment], partner).start()

    for segment in range(2):
        own_rows(segment).start()
    load_labels = pltpu.make_async_copy(labels, label_block, label_sems.at[2])

    barrier = pltpu.get_barrier_semaphore()
    others = [
        (dx, dy, dc) for dy in range(RING) for dx in range(RING) for dc in range(2) if dx or dy or dc
    ]
    with jax.named_scope("barrier"):
        near = [plane(2, 0, 0), plane(1, 0, 0), plane(3, 0, 0), plane(0, 0, 1), *along]
        near += [plane(0, 2, 0), plane(0, 1, 0), plane(0, 3, 0)]
        for device in near:
            pl.semaphore_signal(barrier, inc=1, device_id=device, device_id_type=MESH)
        pl.semaphore_wait(barrier, len(near))

    own_rows(0).wait()
    for dx in (2, 1, 3):
        send_rows(0, dx).start()
    for part in order[:EARLY]:
        send_head(*part).start()
    own_rows(1).wait()
    for dx in (2, 1, 3):
        send_rows(1, dx).start()
    for part in order:
        load_head(*part).start()
    load_labels.start()
    for segment in (2, 4, 3):
        for part in range(2):
            column_rows(segment, part).start()

    label_copy = remote(
        label_rows.at[core], label_rows.at[core], label_sems.at[0], label_sems.at[1], partner
    )

    with jax.named_scope("rows"):
        pass_rows(0)
    for part in order[EARLY:4]:
        send_head(*part).start()
    relay_rows(2)

    def pass_next():
        pass_rows(1)
        for part in order[4:]:
            send_head(*part).start()

    pl.when(core == 1)(jax.named_scope("pass1")(pass_next))
    for k in range(2):
        peaks[k] = jnp.full((2 * block, 128), LOWEST, jnp.float32)
        masses[k] = jnp.zeros((2 * block, 128), jnp.float32)
        picks[k] = jnp.zeros((2 * block, 128), jnp.float32)


    def send_part(t, d, count, which):
        part = pl.ds(0, count)
        if which == 0:
            target, semaphore = first_part.at[t, d, part], first_recv.at[t]
        else:
            target, semaphore = last_parts.at[t, which - 1, d, part], last_recv.at[t]
        device = along[1 - d] if which == 1 else along[d]
        return remote(sent.at[t, which, d, part], target, step_send.at[t], semaphore, device)

    def compute(t, i, segment):
        first, count = span_of(segment)
        early = isinstance(segment, int)

        @pl.when(i == 0)
        @jax.named_scope("wait_rows")
        def _():
            region = row_block(segment, 0, 1 - core, RING)
            arriving(region, pass_recv.at[segment]).wait_recv()

        if early and segment == 0:
            with jax.named_scope("wait_head"):
                here(head_part(core, i, 0, 2), head_local.at[i]).wait()
                arriving(head_part(1 - core, i, 0, 2), head_recv.at[i]).wait_recv()

        for d in range(2):
            result[d, 0 : RING * count, :] = jnp.dot(
                rows[group_of(segment), first * RING : (first + count) * RING, :],
                weights[2 * i + d],
                preferred_element_type=jnp.float32,
            )
            near, far = (1, 3) if d == 0 else (3, 1)
            for which, at in ((0, 0), (1, near * count)):
                for r in range(0, count, 16):
                    sent[t, which, d, r : r + 16, :] = encode(
                        result[d, at + r : at + r + 16, :], code
                    )
                send_part(t, d, count, which).start()
            pending[t, d, 0:count, :] = result[d, far * count : (far + 1) * count, :]
            own[t, d, 0:count, :] = result[d, 2 * count : 3 * count, :]

    def combine(t, i, segment):
        _, count = span_of(segment)
        with jax.named_scope("wait_a"):
            arriving(first_part.at[t, :, pl.ds(0, count)], first_recv.at[t]).wait_recv()
        for d in range(2):
            for r in range(0, count, 16):
                part = slice(r, r + 16)
                sent[t, 2, d, part, :] = encode(
                    pending[t, d, part, :] + decode(first_part[t, d, part, :], code), code
                )
            send_part(t, d, count, 2).start()

    def finish(t, i, segment):
        first, count = span_of(segment)
        source = (y + group_of(segment)) % RING
        which, offset = source // 2, (source % 2) * (block // 2)
        with jax.named_scope("wait_bc"):
            arriving(last_parts.at[t, :, :, pl.ds(0, count)], last_recv.at[t]).wait_recv()
        lane = lax.broadcasted_iota(jnp.int32, (16, 128), 1)
        column = v * (2 * half) + core * half + i * width
        for r in range(0, count, 16):
            token, line = divmod(first + r, block // 2)
            place = pl.ds(pl.multiple_of(token * block + offset + line, 16), 16)
            gap = label_tiles[which, place, :] - lane - column
            tiles = []
            for d in range(2):
                logits = (
                    own[t, d, r : r + 16, :]
                    + decode(last_parts[t, 0, d, r : r + 16, :], code)
                    + decode(last_parts[t, 1, d, r : r + 16, :], code)
                )
                for j in range(0, width, 128):
                    tiles.append((d * CHUNKS * width + j, logits[:, j : j + 128]))
            before = peaks[which, place, :]
            peak = before
            for _, tile in tiles:
                peak = jnp.maximum(peak, tile)
            mass = masses[which, place, :] * jnp.exp(before - peak)
            pick = picks[which, place, :]
            for shift, tile in tiles:
                mass = mass + jnp.exp(tile - peak)
                pick = pick + jnp.where(gap == shift, tile, 0.0)
            peaks[which, place, :] = peak
            masses[which, place, :] = mass
            picks[which, place, :] = pick
        leaving(sent.at[t, :, :, pl.ds(0, count)], step_send.at[t]).wait_send()

    def each(stage, name, t):
        early = (t >= 0) & (t < 2 * CHUNKS)
        is_first = (t < 2) | (t == 4) | (t == 6)

        @pl.when(early & is_first)
        @jax.named_scope(name + "0")
        def _():
            stage(t, jnp.where(t < 2, t, t // 2), 0)

        @pl.when(early & jnp.logical_not(is_first))
        @jax.named_scope(name + "1")
        def _():
            stage(t, jnp.where(t < 4, t - 2, t // 2), 1)

        @pl.when((t >= 2 * CHUNKS) & (t < STEPS))
        @jax.named_scope(name)
        def _():
            stage(t, t % CHUNKS, t // CHUNKS)

    @pl.loop(0, STEPS + LAG_FINAL)
    def _(t):
        each(compute, "compute", t)
        each(combine, "combine", t - LAG_FORWARD)

        @pl.when(t == 2)
        @jax.named_scope("labels")
        def _():
            load_labels.wait()
            label_rows[core, 0:1, 0:block] = label_block[0:1, :]
            label_rows[core, 0:1, block : 2 * block] = label_block[1:2, :]
            label_copy.start()

        @pl.when(t == LAG_FINAL - 1)
        @jax.named_scope("labels")
        def _():
            label_copy.wait()
            for k in range(2):
                label_tiles[k] = jnp.transpose(
                    jnp.broadcast_to(label_rows[k, 0:1, :], (2 * block, 2 * block))
                )

        each(finish, "finish", t - LAG_FINAL)

        @pl.when((t == LATE) & (core == 0))
        @jax.named_scope("pass1")
        def _():
            pass_next()

        for step, stage, segment in (
            (5, relay_rows, 3),
            (6, pass_rows, 2),
            (9, relay_rows, 4),
            (10, pass_rows, 3),
            (14, pass_rows, 4),
        ):

            @pl.when(t == step)
            @jax.named_scope(stage.__name__)
            def _():
                stage(segment)

        @pl.when(t == STEPS)
        @jax.named_scope("drain")
        def _():
            leaving(weights.at[:, pl.ds(0, depth), :], head_send).wait_send()
            for segment in range(RING + 1):
                copies = RING - 1 if segment < 2 else RING
                leaving(row_block(segment, 0, core, copies), row_send.at[segment]).wait_send()
                leaving(row_block(segment, 0, core, RING), pass_send.at[segment]).wait_send()

    with jax.named_scope("reduce"):
        for k in range(2):
            peak_lanes = jnp.transpose(peaks[k])
            peak = jnp.max(peak_lanes, axis=0, keepdims=True)
            mass = jnp.sum(
                jnp.transpose(masses[k]) * jnp.exp(peak_lanes - peak), axis=0, keepdims=True
            )
            pick = jnp.sum(jnp.transpose(picks[k]), axis=0, keepdims=True)
            stats[k, 0:1, :] = peak
            stats[k, 1:2, :] = mass
            stats[k, 2:3, :] = pick
            stats[k, 3:4, :] = jnp.zeros((1, 128), jnp.float32)

    def number(dx, dy, dc):
        return (dx * RING + dy) * 2 + dc

    def send_stats(dx, dy, dc):
        back = number((RING - dx) % RING, (RING - dy) % RING, dc)
        return remote(
            stats.at[(core + dc) % 2],
            all_stats.at[back],
            stat_sems.at[0],
            stat_sems.at[1],
            plane(dx, dy, dc),
        )

    def hops(offset):
        return sum(min(o, RING - o) for o in offset[:2])

    with jax.named_scope("send_stats"):
        for offset in sorted(others, key=hops, reverse=True):
            send_stats(*offset).start()
        all_stats[0] = stats[core]
        leaving(all_stats.at[pl.ds(1, 31)], stat_sems.at[0]).wait_send()

    with jax.named_scope("wait_stats"):
        arriving(all_stats.at[pl.ds(1, 31)], stat_sems.at[1]).wait_recv()

    with jax.named_scope("merge"):
        peak = jnp.max(all_stats[:, 0, :], axis=0, keepdims=True)
        mass = jnp.sum(
            all_stats[:, 1, :] * jnp.exp(all_stats[:, 0, :] - peak), axis=0, keepdims=True
        )
        pick = jnp.sum(all_stats[:, 2, :], axis=0, keepdims=True)
        norm = peak + jnp.log(mass)
        for k in range(2):
            log_norm[k : k + 1, :] = norm[:, k * block : (k + 1) * block]
            picked[k : k + 1, :] = pick[:, k * block : (k + 1) * block]


def body(hidden, head_weight, targets):
    tokens, depth = hidden.shape[1], hidden.shape[2]
    block = 2 * tokens
    width = head_weight.shape[1] // (4 * CHUNKS)
    bound = 800.0 * depth
    code = 32766.0 / math.asinh(bound)
    piece = (2, block, width)
    exact = pltpu.VMEM((STEPS, *piece), jnp.float32)
    lanes = pltpu.VMEM((2, 2 * block, 128), jnp.float32)
    dma = pltpu.SemaphoreType.DMA
    out = jax.ShapeDtypeStruct(targets.shape, jnp.float32)
    vmem = pl.BlockSpec(memory_space=pltpu.VMEM)
    hbm = pl.BlockSpec(memory_space=pltpu.HBM)
    in_hbm = functools.partial(pltpu.with_memory_space_constraint, memory_space=pltpu.HBM)
    log_norm, picked = pl.pallas_call(
        functools.partial(kernel, (block, depth, width, code)),
        out_shape=(out, out),
        in_specs=[hbm, hbm, hbm],
        out_specs=(vmem, vmem),
        scratch_shapes=[
            pltpu.VMEM((2 * CHUNKS, 2 * depth, width), jnp.bfloat16),
            pltpu.VMEM((RING, RING * block, 2 * depth), jnp.bfloat16),
            pltpu.VMEM((2, RING * block, width), jnp.float32),
            pltpu.VMEM((STEPS, 3, *piece), jnp.int16),
            pltpu.VMEM((STEPS, *piece), jnp.int16),
            pltpu.VMEM((STEPS, 2, *piece), jnp.int16),
            exact,
            exact,
            lanes,
            lanes,
            lanes,
            pltpu.VMEM(targets.shape, jnp.int32),
            pltpu.VMEM((2, 8, 2 * block), jnp.int32),
            pltpu.VMEM((2, 2 * block, 128), jnp.int32),
            pltpu.VMEM((2, 4, 128), jnp.float32),
            pltpu.VMEM((32, 4, 128), jnp.float32),
            dma((3,)),
            dma((CHUNKS,)),
            dma((CHUNKS,)),
            dma,
            dma((2,)),
            dma((RING + 1,)),
            dma((RING + 1,)),
            dma((RING + 1,)),
            dma((RING + 1,)),
            dma((RING + 1,)),
            dma((STEPS,)),
            dma((STEPS,)),
            dma((STEPS,)),
            dma((2,)),
        ],
        compiler_params=pltpu.CompilerParams(
            collective_id=0, has_side_effects=True, vmem_limit_bytes=50 * 1024 * 1024
        ),
        name="head_loss",
    )(in_hbm(hidden.reshape(block, depth)), head_weight, in_hbm(targets))
    return log_norm - picked, log_norm * log_norm


def solution(mesh):
    return jax.shard_map(
        body,
        mesh=mesh,
        in_specs=(P(None, "vocab", "hid"), P("hid", "vocab"), P(None, "hid")),
        out_specs=(P(None, "hid"), P(None, "hid")),
        check_vma=False,
    )
```

```python
import functools
import math

import jax
import jax.numpy as jnp
from jax import lax
from jax.experimental import pallas as pl
from jax.experimental.pallas import tpu as pltpu
from jax.sharding import PartitionSpec as P

MESH = pl.DeviceIdType.MESH
RING = 4
CHUNKS = 4
STEPS = (RING + 1) * CHUNKS
FIRST = 32
EARLY = 3
LAG_FORWARD = 3
LAG_FINAL = 7
FIRST_RING, LAST_RING, SEND_RING = 8, 12, 8
LOWEST = -3.0e38


def encode(values, code):
    size = jnp.abs(values)
    square = size * size + 1.0
    level = jnp.log(size + square * lax.rsqrt(square)) * code
    level = jnp.where(values < 0.0, -level, level)
    return jnp.round(level).astype(jnp.int32).astype(jnp.int16)


def decode(codes, code):
    level = codes.astype(jnp.int32).astype(jnp.float32) * (1.0 / code)
    return 0.5 * (jnp.exp(level) - jnp.exp(-level))


def kernel(
    sizes,
    hidden,
    head,
    labels,
    log_norm,
    picked,
    weights,
    rows,
    result,
    sent,
    first_part,
    last_parts,
    own,
    pending,
    peaks,
    masses,
    picks,
    label_block,
    label_rows,
    label_tiles,
    stats,
    all_stats,
    label_sems,
    head_local,
    head_recv,
    head_send,
    own_sem,
    row_send,
    row_recv,
    column_recv,
    pass_send,
    pass_recv,
    step_send,
    first_recv,
    last_recv,
    stat_sems,
):
    block, depth, width, code = sizes
    v, hid = lax.axis_index("vocab"), lax.axis_index("hid")
    x, y = v // RING, v % RING
    z, core = hid // 2, hid % 2
    partner = (v, z * 2 + 1 - core)
    along = ((v, ((z + 1) % RING) * 2 + core), (v, ((z + RING - 1) % RING) * 2 + core))
    slot = (x - z + 2 + RING) % RING
    half = 2 * CHUNKS * width

    def plane(dx, dy, dc):
        return (((x + dx) % RING) * RING + (y + dy) % RING, z * 2 + (core + dc) % 2)

    def remote(source, target, send, recv, device):
        return pltpu.make_async_remote_copy(
            src_ref=source,
            dst_ref=target,
            send_sem=send,
            recv_sem=recv,
            device_id=device,
            device_id_type=MESH,
        )

    def span(segment):
        return (0, FIRST) if segment == 0 else (FIRST, block - FIRST) if segment == 1 else (0, block)

    def group_of(segment):
        return 0 if isinstance(segment, int) and segment < 2 else segment - 1

    def span_of(segment):
        return span(min(segment, 2) if isinstance(segment, int) else 2)

    def row_block(segment, place, which, blocks=1):
        first, count = span_of(segment)
        start = first * RING + place * count
        return rows.at[
            group_of(segment),
            pl.ds(pl.multiple_of(start, 16), blocks * count),
            pl.ds(pl.multiple_of(which * depth, 128), depth),
        ]

    def source_rows(segment):
        first, count = span_of(segment)
        return hidden.at[pl.ds(first, count), :]

    def head_part(which, i, d, parts=1):
        return weights.at[
            pl.ds(2 * i + d, parts), pl.ds(pl.multiple_of(which * depth, 16), depth), :
        ]

    def head_columns(which, i, d):
        start = pl.multiple_of(which * half + (d * CHUNKS + i) * width, 128)
        return head.at[:, pl.ds(start, width)]

    order = [(i, d) for i in range(CHUNKS) for d in range(2)]

    def load_head(i, d):
        return pltpu.make_async_copy(
            head_columns(core, i, d), head_part(core, i, d).at[0], head_local.at[i]
        )

    def send_head(i, d):
        return remote(
            head_columns(1 - core, i, d),
            head_part(core, i, d).at[0],
            head_send,
            head_recv.at[i],
            partner,
        )

    def here(region, semaphore):
        return pltpu.make_async_copy(region, region, semaphore)

    def arriving(region, semaphore):
        return remote(region, region, head_send, semaphore, partner)

    def leaving(region, semaphore):
        return remote(region, region, semaphore, head_recv.at[0], partner)

    def own_rows(segment):
        return pltpu.make_async_copy(
            source_rows(segment), row_block(segment, slot, core), own_sem.at[segment]
        )

    def column_rows(segment, part):
        first, count = span(part)
        return remote(
            row_block(part, slot, core),
            rows.at[
                group_of(segment),
                pl.ds(pl.multiple_of(slot * block + first, 16), count),
                pl.ds(pl.multiple_of(core * depth, 128), depth),
            ],
            row_send.at[segment],
            column_recv.at[segment],
            plane(0, RING + 1 - segment, 0),
        )

    def send_rows(segment, dx):
        there = row_block(segment, slot, core)
        return remote(
            there,
            there,
            row_send.at[segment],
            row_recv.at[segment],
            plane(dx, 0, 0),
        )

    def relay_rows(segment):
        there = row_block(segment, slot, core)
        arriving(there, column_recv.at[segment]).wait_recv()
        for dx in (2, 1, 3):
            send_rows(segment, dx).start()

    def pass_rows(segment):
        arriving(row_block(segment, 0, core, RING - 1), row_recv.at[segment]).wait_recv()
        there = row_block(segment, 0, core, RING)
        remote(there, there, pass_send.at[segment], pass_recv.at[segment], partner).start()

    for segment in range(2):
        own_rows(segment).start()
    load_labels = pltpu.make_async_copy(labels, label_block, label_sems.at[2])

    barrier = pltpu.get_barrier_semaphore()
    others = [
        (dx, dy, dc) for dy in range(RING) for dx in range(RING) for dc in range(2) if dx or dy or dc
    ]
    with jax.named_scope("barrier"):
        near = [plane(2, 0, 0), plane(1, 0, 0), plane(3, 0, 0), plane(0, 0, 1), *along]
        near += [plane(0, 2, 0), plane(0, 1, 0), plane(0, 3, 0)]
        for device in near:
            pl.semaphore_signal(barrier, inc=1, device_id=device, device_id_type=MESH)
        pl.semaphore_wait(barrier, len(near))

    own_rows(0).wait()
    for dx in (2, 1, 3):
        send_rows(0, dx).start()
    for part in order[:EARLY]:
        send_head(*part).start()
    own_rows(1).wait()

    def send_next():
        for dx in (2, 1, 3):
            send_rows(1, dx).start()

    pl.when(core == 0)(send_next)
    for part in order:
        load_head(*part).start()
    load_labels.start()
    for segment in (2, 4, 3):
        for part in range(2):
            column_rows(segment, part).start()

    label_copy = remote(
        label_rows.at[core], label_rows.at[core], label_sems.at[0], label_sems.at[1], partner
    )

    with jax.named_scope("rows"):
        pass_rows(0)
    pl.when(core == 1)(send_next)
    for part in order[EARLY:4]:
        send_head(*part).start()

    def pass_next():
        pass_rows(1)
        for part in order[4:]:
            send_head(*part).start()

    for k in range(2):
        peaks[k] = jnp.full((2 * block, 128), LOWEST, jnp.float32)
        masses[k] = jnp.zeros((2 * block, 128), jnp.float32)
        picks[k] = jnp.zeros((2 * block, 128), jnp.float32)


    def send_part(t, d, count, which):
        part = pl.ds(0, count)
        if which == 0:
            target, semaphore = first_part.at[t, d, part], first_recv.at[t % FIRST_RING]
        else:
            target = last_parts.at[t, which - 1, d, part]
            semaphore = last_recv.at[t % LAST_RING]
        device = along[1 - d] if which == 1 else along[d]
        leave = step_send.at[t % SEND_RING]
        return remote(sent.at[t, which, d, part], target, leave, semaphore, device)

    def compute(t, i, segment):
        first, count = span_of(segment)
        early = isinstance(segment, int)

        @pl.when(i == 0)
        @jax.named_scope("wait_rows")
        def _():
            region = row_block(segment, 0, 1 - core, RING)
            arriving(region, pass_recv.at[segment]).wait_recv()

        if early and segment == 0:
            with jax.named_scope("wait_head"):
                here(head_part(core, i, 0, 2), head_local.at[i]).wait()
                arriving(head_part(1 - core, i, 0, 2), head_recv.at[i]).wait_recv()

        for d in range(2):
            result[d, 0 : RING * count, :] = jnp.dot(
                rows[group_of(segment), first * RING : (first + count) * RING, :],
                weights[2 * i + d],
                preferred_element_type=jnp.float32,
            )
            near, far = (1, 3) if d == 0 else (3, 1)
            for which, at in ((0, 0), (1, near * count)):
                for r in range(0, count, 16):
                    sent[t, which, d, r : r + 16, :] = encode(
                        result[d, at + r : at + r + 16, :], code
                    )
                send_part(t, d, count, which).start()
            pending[t, d, 0:count, :] = result[d, far * count : (far + 1) * count, :]
            own[t, d, 0:count, :] = result[d, 2 * count : 3 * count, :]

    def combine(t, i, segment):
        _, count = span_of(segment)
        with jax.named_scope("wait_a"):
            arriving(first_part.at[t, :, pl.ds(0, count)], first_recv.at[t % FIRST_RING]).wait_recv()
        for d in range(2):
            for r in range(0, count, 16):
                part = slice(r, r + 16)
                sent[t, 2, d, part, :] = encode(
                    pending[t, d, part, :] + decode(first_part[t, d, part, :], code), code
                )
            send_part(t, d, count, 2).start()

    def finish(t, i, segment):
        first, count = span_of(segment)
        source = (y + group_of(segment)) % RING
        which, offset = source // 2, (source % 2) * (block // 2)
        with jax.named_scope("wait_bc"):
            region = last_parts.at[t, :, :, pl.ds(0, count)]
            arriving(region, last_recv.at[t % LAST_RING]).wait_recv()
        lane = lax.broadcasted_iota(jnp.int32, (16, 128), 1)
        column = v * (2 * half) + core * half + i * width
        for r in range(0, count, 16):
            token, line = divmod(first + r, block // 2)
            place = pl.ds(pl.multiple_of(token * block + offset + line, 16), 16)
            gap = label_tiles[which, place, :] - lane - column
            tiles = []
            for d in range(2):
                logits = (
                    own[t, d, r : r + 16, :]
                    + decode(last_parts[t, 0, d, r : r + 16, :], code)
                    + decode(last_parts[t, 1, d, r : r + 16, :], code)
                )
                for j in range(0, width, 128):
                    tiles.append((d * CHUNKS * width + j, logits[:, j : j + 128]))
            before = peaks[which, place, :]
            peak = before
            for _, tile in tiles:
                peak = jnp.maximum(peak, tile)
            mass = masses[which, place, :] * jnp.exp(before - peak)
            pick = picks[which, place, :]
            for shift, tile in tiles:
                mass = mass + jnp.exp(tile - peak)
                pick = pick + jnp.where(gap == shift, tile, 0.0)
            peaks[which, place, :] = peak
            masses[which, place, :] = mass
            picks[which, place, :] = pick
        leaving(sent.at[t, :, :, pl.ds(0, count)], step_send.at[t % SEND_RING]).wait_send()

    def each(stage, name, t):
        early = (t >= 0) & (t < 2 * CHUNKS)
        is_first = (t < 2) | (t == 4) | (t == 6)

        @pl.when(early & is_first)
        @jax.named_scope(name + "0")
        def _():
            stage(t, jnp.where(t < 2, t, t // 2), 0)

        @pl.when(early & jnp.logical_not(is_first))
        @jax.named_scope(name + "1")
        def _():
            stage(t, jnp.where(t < 4, t - 2, t // 2), 1)

        @pl.when((t >= 2 * CHUNKS) & (t < STEPS))
        @jax.named_scope(name)
        def _():
            stage(t, t % CHUNKS, t // CHUNKS)

    @pl.loop(0, STEPS + LAG_FINAL)
    def _(t):
        each(compute, "compute", t)
        each(combine, "combine", t - LAG_FORWARD)

        @pl.when(t == 2)
        @jax.named_scope("labels")
        def _():
            load_labels.wait()
            label_rows[core, 0:1, 0:block] = label_block[0:1, :]
            label_rows[core, 0:1, block : 2 * block] = label_block[1:2, :]
            label_copy.start()

        @pl.when(t == LAG_FINAL - 1)
        @jax.named_scope("labels")
        def _():
            label_copy.wait()
            for k in range(2):
                label_tiles[k] = jnp.transpose(
                    jnp.broadcast_to(label_rows[k, 0:1, :], (2 * block, 2 * block))
                )

        each(finish, "finish", t - LAG_FINAL)

        @pl.when(t == 0)
        @jax.named_scope("pass1")
        def _():
            pass_next()

        for step, stage, segment in (
            (2, relay_rows, 2),
            (5, relay_rows, 3),
            (7, pass_rows, 2),
            (9, relay_rows, 4),
            (10, pass_rows, 3),
            (14, pass_rows, 4),
        ):

            @pl.when(t == step)
            @jax.named_scope(stage.__name__)
            def _():
                stage(segment)

        @pl.when(t == STEPS)
        @jax.named_scope("drain")
        def _():
            leaving(weights.at[:, pl.ds(0, depth), :], head_send).wait_send()
            for segment in range(RING + 1):
                copies = RING - 1 if segment < 2 else RING
                leaving(row_block(segment, 0, core, copies), row_send.at[segment]).wait_send()
                leaving(row_block(segment, 0, core, RING), pass_send.at[segment]).wait_send()

    with jax.named_scope("reduce"):
        for k in range(2):
            peak_lanes = jnp.transpose(peaks[k])
            peak = jnp.max(peak_lanes, axis=0, keepdims=True)
            mass = jnp.sum(
                jnp.transpose(masses[k]) * jnp.exp(peak_lanes - peak), axis=0, keepdims=True
            )
            pick = jnp.sum(jnp.transpose(picks[k]), axis=0, keepdims=True)
            stats[k, 0:1, :] = peak
            stats[k, 1:2, :] = mass
            stats[k, 2:3, :] = pick
            stats[k, 3:4, :] = jnp.zeros((1, 128), jnp.float32)

    def number(dx, dy, dc):
        return (dx * RING + dy) * 2 + dc

    def send_stats(dx, dy, dc):
        back = number((RING - dx) % RING, (RING - dy) % RING, dc)
        return remote(
            stats.at[(core + dc) % 2],
            all_stats.at[back],
            stat_sems.at[0],
            stat_sems.at[1],
            plane(dx, dy, dc),
        )

    def hops(offset):
        return sum(min(o, RING - o) for o in offset[:2])

    with jax.named_scope("send_stats"):
        for offset in sorted(others, key=hops, reverse=True):
            send_stats(*offset).start()
        all_stats[0] = stats[core]
        leaving(all_stats.at[pl.ds(1, 31)], stat_sems.at[0]).wait_send()

    with jax.named_scope("wait_stats"):
        arriving(all_stats.at[pl.ds(1, 31)], stat_sems.at[1]).wait_recv()

    with jax.named_scope("merge"):
        peak = jnp.max(all_stats[:, 0, :], axis=0, keepdims=True)
        mass = jnp.sum(
            all_stats[:, 1, :] * jnp.exp(all_stats[:, 0, :] - peak), axis=0, keepdims=True
        )
        pick = jnp.sum(all_stats[:, 2, :], axis=0, keepdims=True)
        norm = peak + jnp.log(mass)
        for k in range(2):
            log_norm[k : k + 1, :] = norm[:, k * block : (k + 1) * block]
            picked[k : k + 1, :] = pick[:, k * block : (k + 1) * block]


def body(hidden, head_weight, targets):
    tokens, depth = hidden.shape[1], hidden.shape[2]
    block = 2 * tokens
    width = head_weight.shape[1] // (4 * CHUNKS)
    bound = 800.0 * depth
    code = 32766.0 / math.asinh(bound)
    piece = (2, block, width)
    exact = pltpu.VMEM((STEPS, *piece), jnp.float32)
    lanes = pltpu.VMEM((2, 2 * block, 128), jnp.float32)
    dma = pltpu.SemaphoreType.DMA
    out = jax.ShapeDtypeStruct(targets.shape, jnp.float32)
    vmem = pl.BlockSpec(memory_space=pltpu.VMEM)
    hbm = pl.BlockSpec(memory_space=pltpu.HBM)
    in_hbm = functools.partial(pltpu.with_memory_space_constraint, memory_space=pltpu.HBM)
    log_norm, picked = pl.pallas_call(
        functools.partial(kernel, (block, depth, width, code)),
        out_shape=(out, out),
        in_specs=[hbm, hbm, hbm],
        out_specs=(vmem, vmem),
        scratch_shapes=[
            pltpu.VMEM((2 * CHUNKS, 2 * depth, width), jnp.bfloat16),
            pltpu.VMEM((RING, RING * block, 2 * depth), jnp.bfloat16),
            pltpu.VMEM((2, RING * block, width), jnp.float32),
            pltpu.VMEM((STEPS, 3, *piece), jnp.int16),
            pltpu.VMEM((STEPS, *piece), jnp.int16),
            pltpu.VMEM((STEPS, 2, *piece), jnp.int16),
            exact,
            exact,
            lanes,
            lanes,
            lanes,
            pltpu.VMEM(targets.shape, jnp.int32),
            pltpu.VMEM((2, 8, 2 * block), jnp.int32),
            pltpu.VMEM((2, 2 * block, 128), jnp.int32),
            pltpu.VMEM((2, 4, 128), jnp.float32),
            pltpu.VMEM((32, 4, 128), jnp.float32),
            dma((3,)),
            dma((CHUNKS,)),
            dma((CHUNKS,)),
            dma,
            dma((2,)),
            dma((RING + 1,)),
            dma((RING + 1,)),
            dma((RING + 1,)),
            dma((RING + 1,)),
            dma((RING + 1,)),
            dma((SEND_RING,)),
            dma((FIRST_RING,)),
            dma((LAST_RING,)),
            dma((2,)),
        ],
        compiler_params=pltpu.CompilerParams(
            collective_id=0, has_side_effects=True, vmem_limit_bytes=50 * 1024 * 1024
        ),
        name="head_loss",
    )(in_hbm(hidden.reshape(block, depth)), head_weight, in_hbm(targets))
    return log_norm - picked, log_norm * log_norm


def solution(mesh):
    return jax.shard_map(
        body,
        mesh=mesh,
        in_specs=(P(None, "vocab", "hid"), P("hid", "vocab"), P(None, "hid")),
        out_specs=(P(None, "hid"), P(None, "hid")),
        check_vma=False,
    )
```

```python
import functools
import math

import jax
import jax.numpy as jnp
from jax import lax
from jax.experimental import pallas as pl
from jax.experimental.pallas import tpu as pltpu
from jax.sharding import PartitionSpec as P

MESH = pl.DeviceIdType.MESH
RING = 4
CHUNKS = 4
STEPS = (RING + 1) * CHUNKS
FIRST = 32
EARLY = 3
LAG_FORWARD = 3
LAG_FINAL = 7
FIRST_RING, LAST_RING, SEND_RING = 8, 12, 8
LOWEST = -3.0e38


def encode(values, code):
    size = jnp.abs(values)
    square = size * size + 1.0
    level = jnp.log(size + square * lax.rsqrt(square)) * code
    level = jnp.where(values < 0.0, -level, level)
    return jnp.round(level).astype(jnp.int32).astype(jnp.int16)


def decode(codes, code):
    level = codes.astype(jnp.int32).astype(jnp.float32) * (1.0 / code)
    return 0.5 * (jnp.exp(level) - jnp.exp(-level))


def kernel(
    sizes,
    hidden,
    head,
    labels,
    log_norm,
    picked,
    weights,
    rows,
    result,
    sent,
    first_part,
    last_parts,
    own,
    pending,
    peaks,
    masses,
    picks,
    label_block,
    label_rows,
    label_tiles,
    stats,
    all_stats,
    label_sems,
    head_local,
    head_recv,
    head_send,
    own_sem,
    row_send,
    row_recv,
    column_recv,
    pass_send,
    pass_recv,
    step_send,
    first_recv,
    last_recv,
    stat_sems,
):
    block, depth, width, code = sizes
    v, hid = lax.axis_index("vocab"), lax.axis_index("hid")
    x, y = v // RING, v % RING
    z, core = hid // 2, hid % 2
    partner = (v, z * 2 + 1 - core)
    along = ((v, ((z + 1) % RING) * 2 + core), (v, ((z + RING - 1) % RING) * 2 + core))
    slot = (x - z + 2 + RING) % RING
    half = 2 * CHUNKS * width

    def plane(dx, dy, dc):
        return (((x + dx) % RING) * RING + (y + dy) % RING, z * 2 + (core + dc) % 2)

    def remote(source, target, send, recv, device):
        return pltpu.make_async_remote_copy(
            src_ref=source,
            dst_ref=target,
            send_sem=send,
            recv_sem=recv,
            device_id=device,
            device_id_type=MESH,
        )

    def span(segment):
        return (0, FIRST) if segment == 0 else (FIRST, block - FIRST) if segment == 1 else (0, block)

    def group_of(segment):
        return 0 if isinstance(segment, int) and segment < 2 else segment - 1

    def span_of(segment):
        return span(min(segment, 2) if isinstance(segment, int) else 2)

    def row_block(segment, place, which, blocks=1):
        first, count = span_of(segment)
        start = first * RING + place * count
        return rows.at[
            group_of(segment),
            pl.ds(pl.multiple_of(start, 16), blocks * count),
            pl.ds(pl.multiple_of(which * depth, 128), depth),
        ]

    def source_rows(segment):
        first, count = span_of(segment)
        return hidden.at[pl.ds(first, count), :]

    def head_part(which, i, d, parts=1):
        return weights.at[
            pl.ds(2 * i + d, parts), pl.ds(pl.multiple_of(which * depth, 16), depth), :
        ]

    def head_columns(which, i, d):
        start = pl.multiple_of(which * half + (d * CHUNKS + i) * width, 128)
        return head.at[:, pl.ds(start, width)]

    order = [(i, d) for i in range(CHUNKS) for d in range(2)]

    def load_head(i, d):
        return pltpu.make_async_copy(
            head_columns(core, i, d), head_part(core, i, d).at[0], head_local.at[i]
        )

    def send_head(i, d):
        return remote(
            head_columns(1 - core, i, d),
            head_part(core, i, d).at[0],
            head_send,
            head_recv.at[i],
            partner,
        )

    def here(region, semaphore):
        return pltpu.make_async_copy(region, region, semaphore)

    def arriving(region, semaphore):
        return remote(region, region, head_send, semaphore, partner)

    def leaving(region, semaphore):
        return remote(region, region, semaphore, head_recv.at[0], partner)

    def own_rows(segment):
        return pltpu.make_async_copy(
            source_rows(segment), row_block(segment, slot, core), own_sem.at[segment]
        )

    def column_rows(segment, part):
        first, count = span(part)
        return remote(
            row_block(part, slot, core),
            rows.at[
                group_of(segment),
                pl.ds(pl.multiple_of(slot * block + first, 16), count),
                pl.ds(pl.multiple_of(core * depth, 128), depth),
            ],
            row_send.at[0 if segment < 2 else 1],
            column_recv.at[segment - 2],
            plane(0, RING + 1 - segment, 0),
        )

    def send_rows(segment, dx):
        there = row_block(segment, slot, core)
        return remote(
            there,
            there,
            row_send.at[0 if segment < 2 else 1],
            row_recv.at[segment],
            plane(dx, 0, 0),
        )

    def relay_rows(segment):
        there = row_block(segment, slot, core)
        arriving(there, column_recv.at[segment - 2]).wait_recv()
        for dx in (2, 1, 3):
            send_rows(segment, dx).start()

    def pass_rows(segment):
        arriving(row_block(segment, 0, core, RING - 1), row_recv.at[segment]).wait_recv()
        there = row_block(segment, 0, core, RING)
        remote(there, there, pass_send, pass_recv.at[segment], partner).start()

    for segment in range(2):
        own_rows(segment).start()
    load_labels = pltpu.make_async_copy(labels, label_block, label_sems.at[2])

    barrier = pltpu.get_barrier_semaphore()
    others = [
        (dx, dy, dc) for dy in range(RING) for dx in range(RING) for dc in range(2) if dx or dy or dc
    ]
    with jax.named_scope("barrier"):
        near = [plane(2, 0, 0), plane(1, 0, 0), plane(3, 0, 0), plane(0, 0, 1), *along]
        near += [plane(0, 2, 0), plane(0, 1, 0), plane(0, 3, 0)]
        for device in near:
            pl.semaphore_signal(barrier, inc=1, device_id=device, device_id_type=MESH)
        pl.semaphore_wait(barrier, len(near))

    own_rows(0).wait()
    for dx in (2, 1, 3):
        send_rows(0, dx).start()
    for part in order[:EARLY]:
        send_head(*part).start()
    own_rows(1).wait()

    def send_next():
        for dx in (2, 1, 3):
            send_rows(1, dx).start()

    pl.when(core == 0)(send_next)
    for part in order:
        load_head(*part).start()
    load_labels.start()
    label_copy = remote(
        label_rows.at[core], label_rows.at[core], label_sems.at[0], label_sems.at[1], partner
    )

    with jax.named_scope("rows"):
        pass_rows(0)
    pl.when(core == 1)(send_next)
    for segment in (2, 4, 3):
        for part in range(2):
            column_rows(segment, part).start()

    for part in order[EARLY:4]:
        send_head(*part).start()

    def pass_next():
        pass_rows(1)
        for part in order[4:]:
            send_head(*part).start()

    for k in range(2):
        peaks[k] = jnp.full((2 * block, 128), LOWEST, jnp.float32)
        masses[k] = jnp.zeros((2 * block, 128), jnp.float32)
        picks[k] = jnp.zeros((2 * block, 128), jnp.float32)


    def send_part(t, d, count, which):
        part = pl.ds(0, count)
        if which == 0:
            target, semaphore = first_part.at[t, d, part], first_recv.at[t % FIRST_RING]
        else:
            target = last_parts.at[t, which - 1, d, part]
            semaphore = last_recv.at[t % LAST_RING]
        device = along[1 - d] if which == 1 else along[d]
        leave = step_send.at[t % SEND_RING]
        return remote(sent.at[t, which, d, part], target, leave, semaphore, device)

    def compute(t, i, segment):
        first, count = span_of(segment)
        early = isinstance(segment, int)

        @pl.when(i == 0)
        @jax.named_scope("wait_rows")
        def _():
            region = row_block(segment, 0, 1 - core, RING)
            arriving(region, pass_recv.at[segment]).wait_recv()

        if early and segment == 0:
            with jax.named_scope("wait_head"):
                here(head_part(core, i, 0, 2), head_local.at[i]).wait()
                arriving(head_part(1 - core, i, 0, 2), head_recv.at[i]).wait_recv()

        for d in range(2):
            result[d, 0 : RING * count, :] = jnp.dot(
                rows[group_of(segment), first * RING : (first + count) * RING, :],
                weights[2 * i + d],
                preferred_element_type=jnp.float32,
            )
            near, far = (1, 3) if d == 0 else (3, 1)
            for which, at in ((0, 0), (1, near * count)):
                for r in range(0, count, 16):
                    sent[t, which, d, r : r + 16, :] = encode(
                        result[d, at + r : at + r + 16, :], code
                    )
                send_part(t, d, count, which).start()
            pending[t, d, 0:count, :] = result[d, far * count : (far + 1) * count, :]
            own[t, d, 0:count, :] = result[d, 2 * count : 3 * count, :]

    def combine(t, i, segment):
        _, count = span_of(segment)
        with jax.named_scope("wait_a"):
            arriving(first_part.at[t, :, pl.ds(0, count)], first_recv.at[t % FIRST_RING]).wait_recv()
        for d in range(2):
            for r in range(0, count, 16):
                part = slice(r, r + 16)
                sent[t, 2, d, part, :] = encode(
                    pending[t, d, part, :] + decode(first_part[t, d, part, :], code), code
                )
            send_part(t, d, count, 2).start()

    def finish(t, i, segment):
        first, count = span_of(segment)
        source = (y + group_of(segment)) % RING
        which, offset = source // 2, (source % 2) * (block // 2)
        with jax.named_scope("wait_bc"):
            region = last_parts.at[t, :, :, pl.ds(0, count)]
            arriving(region, last_recv.at[t % LAST_RING]).wait_recv()
        lane = lax.broadcasted_iota(jnp.int32, (16, 128), 1)
        column = v * (2 * half) + core * half + i * width
        for r in range(0, count, 16):
            token, line = divmod(first + r, block // 2)
            place = pl.ds(pl.multiple_of(token * block + offset + line, 16), 16)
            gap = label_tiles[which, place, :] - lane - column
            tiles = []
            for d in range(2):
                logits = (
                    own[t, d, r : r + 16, :]
                    + decode(last_parts[t, 0, d, r : r + 16, :], code)
                    + decode(last_parts[t, 1, d, r : r + 16, :], code)
                )
                for j in range(0, width, 128):
                    tiles.append((d * CHUNKS * width + j, logits[:, j : j + 128]))
            before = peaks[which, place, :]
            peak = before
            for _, tile in tiles:
                peak = jnp.maximum(peak, tile)
            mass = masses[which, place, :] * jnp.exp(before - peak)
            pick = picks[which, place, :]
            for shift, tile in tiles:
                mass = mass + jnp.exp(tile - peak)
                pick = pick + jnp.where(gap == shift, tile, 0.0)
            peaks[which, place, :] = peak
            masses[which, place, :] = mass
            picks[which, place, :] = pick
        leaving(sent.at[t, :, :, pl.ds(0, count)], step_send.at[t % SEND_RING]).wait_send()

    def each(stage, name, t):
        early = (t >= 0) & (t < 2 * CHUNKS)
        is_first = (t < 2) | (t == 4) | (t == 6)

        @pl.when(early & is_first)
        @jax.named_scope(name + "0")
        def _():
            stage(t, jnp.where(t < 2, t, t // 2), 0)

        @pl.when(early & jnp.logical_not(is_first))
        @jax.named_scope(name + "1")
        def _():
            stage(t, jnp.where(t < 4, t - 2, t // 2), 1)

        @pl.when((t >= 2 * CHUNKS) & (t < STEPS))
        @jax.named_scope(name)
        def _():
            stage(t, t % CHUNKS, t // CHUNKS)

    @pl.loop(0, STEPS + LAG_FINAL)
    def _(t):
        each(compute, "compute", t)
        each(combine, "combine", t - LAG_FORWARD)

        @pl.when(t == 2)
        @jax.named_scope("labels")
        def _():
            load_labels.wait()
            label_rows[core, 0:1, 0:block] = label_block[0:1, :]
            label_rows[core, 0:1, block : 2 * block] = label_block[1:2, :]
            label_copy.start()

        @pl.when(t == LAG_FINAL - 1)
        @jax.named_scope("labels")
        def _():
            label_copy.wait()
            for k in range(2):
                label_tiles[k] = jnp.transpose(
                    jnp.broadcast_to(label_rows[k, 0:1, :], (2 * block, 2 * block))
                )

        each(finish, "finish", t - LAG_FINAL)

        @pl.when(t == 0)
        @jax.named_scope("pass1")
        def _():
            pass_next()

        for step, stage, segment in (
            (2, relay_rows, 2),
            (5, relay_rows, 3),
            (7, pass_rows, 2),
            (9, relay_rows, 4),
            (10, pass_rows, 3),
            (14, pass_rows, 4),
        ):

            @pl.when(t == step)
            @jax.named_scope(stage.__name__)
            def _():
                stage(segment)

        @pl.when(t == STEPS)
        @jax.named_scope("drain")
        def _():
            leaving(weights.at[:, pl.ds(0, depth), :], head_send).wait_send()
            mine = pl.ds(pl.multiple_of(core * depth, 128), depth)
            leaving(rows.at[0, pl.ds(0, 3 * block), mine], row_send.at[0]).wait_send()
            leaving(rows.at[pl.ds(0, RING - 1), :, mine], row_send.at[1]).wait_send()
            leaving(rows.at[:, :, mine], pass_send).wait_send()

    with jax.named_scope("reduce"):
        for k in range(2):
            peak_lanes = jnp.transpose(peaks[k])
            peak = jnp.max(peak_lanes, axis=0, keepdims=True)
            mass = jnp.sum(
                jnp.transpose(masses[k]) * jnp.exp(peak_lanes - peak), axis=0, keepdims=True
            )
            pick = jnp.sum(jnp.transpose(picks[k]), axis=0, keepdims=True)
            stats[k, 0:1, :] = peak
            stats[k, 1:2, :] = mass
            stats[k, 2:3, :] = pick
            stats[k, 3:4, :] = jnp.zeros((1, 128), jnp.float32)

    def number(dx, dy, dc):
        return (dx * RING + dy) * 2 + dc

    def send_stats(dx, dy, dc):
        back = number((RING - dx) % RING, (RING - dy) % RING, dc)
        return remote(
            stats.at[(core + dc) % 2],
            all_stats.at[back],
            stat_sems.at[0],
            stat_sems.at[1],
            plane(dx, dy, dc),
        )

    def hops(offset):
        return sum(min(o, RING - o) for o in offset[:2])

    with jax.named_scope("send_stats"):
        for offset in sorted(others, key=hops, reverse=True):
            send_stats(*offset).start()
        all_stats[0] = stats[core]
        leaving(all_stats.at[pl.ds(1, 31)], stat_sems.at[0]).wait_send()

    with jax.named_scope("wait_stats"):
        arriving(all_stats.at[pl.ds(1, 31)], stat_sems.at[1]).wait_recv()

    with jax.named_scope("merge"):
        peak = jnp.max(all_stats[:, 0, :], axis=0, keepdims=True)
        mass = jnp.sum(
            all_stats[:, 1, :] * jnp.exp(all_stats[:, 0, :] - peak), axis=0, keepdims=True
        )
        pick = jnp.sum(all_stats[:, 2, :], axis=0, keepdims=True)
        norm = peak + jnp.log(mass)
        for k in range(2):
            log_norm[k : k + 1, :] = norm[:, k * block : (k + 1) * block]
            picked[k : k + 1, :] = pick[:, k * block : (k + 1) * block]


def body(hidden, head_weight, targets):
    tokens, depth = hidden.shape[1], hidden.shape[2]
    block = 2 * tokens
    width = head_weight.shape[1] // (4 * CHUNKS)
    bound = 800.0 * depth
    code = 32766.0 / math.asinh(bound)
    piece = (2, block, width)
    exact = pltpu.VMEM((STEPS, *piece), jnp.float32)
    lanes = pltpu.VMEM((2, 2 * block, 128), jnp.float32)
    dma = pltpu.SemaphoreType.DMA
    out = jax.ShapeDtypeStruct(targets.shape, jnp.float32)
    vmem = pl.BlockSpec(memory_space=pltpu.VMEM)
    hbm = pl.BlockSpec(memory_space=pltpu.HBM)
    in_hbm = functools.partial(pltpu.with_memory_space_constraint, memory_space=pltpu.HBM)
    log_norm, picked = pl.pallas_call(
        functools.partial(kernel, (block, depth, width, code)),
        out_shape=(out, out),
        in_specs=[hbm, hbm, hbm],
        out_specs=(vmem, vmem),
        scratch_shapes=[
            pltpu.VMEM((2 * CHUNKS, 2 * depth, width), jnp.bfloat16),
            pltpu.VMEM((RING, RING * block, 2 * depth), jnp.bfloat16),
            pltpu.VMEM((2, RING * block, width), jnp.float32),
            pltpu.VMEM((STEPS, 3, *piece), jnp.int16),
            pltpu.VMEM((STEPS, *piece), jnp.int16),
            pltpu.VMEM((STEPS, 2, *piece), jnp.int16),
            exact,
            exact,
            lanes,
            lanes,
            lanes,
            pltpu.VMEM(targets.shape, jnp.int32),
            pltpu.VMEM((2, 8, 2 * block), jnp.int32),
            pltpu.VMEM((2, 2 * block, 128), jnp.int32),
            pltpu.VMEM((2, 4, 128), jnp.float32),
            pltpu.VMEM((32, 4, 128), jnp.float32),
            dma((3,)),
            dma((CHUNKS,)),
            dma((CHUNKS,)),
            dma,
            dma((2,)),
            dma((2,)),
            dma((RING + 1,)),
            dma((RING - 1,)),
            dma,
            dma((RING + 1,)),
            dma((SEND_RING,)),
            dma((FIRST_RING,)),
            dma((LAST_RING,)),
            dma((2,)),
        ],
        compiler_params=pltpu.CompilerParams(
            collective_id=0, has_side_effects=True, vmem_limit_bytes=50 * 1024 * 1024
        ),
        name="head_loss",
    )(in_hbm(hidden.reshape(block, depth)), head_weight, in_hbm(targets))
    return log_norm - picked, log_norm * log_norm


def solution(mesh):
    return jax.shard_map(
        body,
        mesh=mesh,
        in_specs=(P(None, "vocab", "hid"), P("hid", "vocab"), P(None, "hid")),
        out_specs=(P(None, "hid"), P(None, "hid")),
        check_vma=False,
    )
```
